64 devices in a mesh: rep: 4 (over x, y), dp: 16 (over z, core).
Axes of the slice: x: 2, y: 2, z: 8, core: 2. Of those that a mesh axis runs over, the one named last changes fastest.
The devices are a block of a 4x4x8 slice.
Arguments:
- hidden: bfloat16 [2048, 5120], P(('rep', 'dp')), parts along dimension 0
- ckv_cache: bfloat16 [2048, 256, 512], P(('rep', 'dp')), parts along dimension 0
- kpe_cache: bfloat16 [2048, 256, 64], P(('rep', 'dp')), parts along dimension 0
- cache_len: int32 [2048], P(('rep', 'dp')), parts along dimension 0
- rope_cos: float32 [2048, 32], P(('rep', 'dp')), parts along dimension 0
- rope_sin: float32 [2048, 32], P(('rep', 'dp')), parts along dimension 0
- norm_attn: float32 [5120], replicated
- w_dq: bfloat16 [5120, 1536], replicated
- norm_q: float32 [1536], replicated
- w_uq: bfloat16 [1536, 128, 192], replicated
- w_dkv: bfloat16 [5120, 576], replicated
- norm_kv: float32 [512], replicated
- w_uk: bfloat16 [512, 128, 128], replicated
- w_uv: bfloat16 [512, 128, 128], replicated
- w_out: bfloat16 [128, 128, 5120], replicated
- norm_mlp: float32 [5120], replicated
- w_gate: bfloat16 [5120, 12288], P(None, 'dp')
- w_up: bfloat16 [5120, 12288], P(None, 'dp')
- w_down: bfloat16 [12288, 5120], P('dp')
Outputs:
- output 1: bfloat16 [2048, 5120], P(('rep', 'dp')), parts along dimension 0
- output 2: bfloat16 [2048, 512], P(('rep', 'dp')), parts along dimension 0
- output 3: bfloat16 [2048, 64], P(('rep', 'dp')), parts along dimension 0
There are 4 independent parts. The reference program is written for one: setup_inputs(seed, part) draws one part's arguments, and reference() takes and returns one part's arrays. A program takes and returns all parts, laid end to end along the dimension named above; an argument that names none is the same for every part.
All inputs are finite; a program needn't handle non-finite values.
Results may differ from the reference program's by a relative error of at most 0.0108911.
Values are sent between devices in bfloat16 or wider.
A program may use at most 768 MiB of HBM per device.

```python
import math
import jax
import jax.numpy as jnp
from jax import lax

BATCH = 512
SEQ_LEN = 256
D_MODEL = 5120
HEADS = 128
Q_LORA = 1536
KV_LORA = 512
NOPE_DIM = 128
ROPE_DIM = 64
V_HEAD = 128
FF_DIM = 12288

EPSILON = 1e-6
MSCALE = 0.1 * math.log(40.0) + 1.0
SCORE_SCALE = MSCALE * MSCALE / math.sqrt(NOPE_DIM + ROPE_DIM)


def weight_draw(rand_key, arr_shape, fan_in):
    return (jax.random.normal(rand_key, arr_shape, jnp.float32) * fan_in ** -0.5).astype(jnp.bfloat16)


def gain_draw(rand_key, vec_size):
    return 1.0 + 0.3 * jax.random.normal(rand_key, (vec_size,), jnp.float32)


def setup_inputs(seed: int = 0, part: int = 0) -> dict:
    base_key = jax.random.key(seed)
    shared_keys = jax.random.split(base_key, 16)
    part_keys = jax.random.split(jax.random.fold_in(base_key, part), 8)
    half_rope = ROPE_DIM // 2
    hidden = jax.random.normal(part_keys[0], (BATCH, D_MODEL), jnp.float32).astype(jnp.bfloat16)
    centre = jax.random.normal(part_keys[1], (BATCH, 1, KV_LORA), jnp.float32)
    spread = jax.random.normal(part_keys[2], (BATCH, SEQ_LEN, KV_LORA), jnp.float32)
    ckv_cache = (0.6 * centre + 0.8 * spread).astype(jnp.bfloat16)
    kpe_cache = jax.random.normal(part_keys[3], (BATCH, SEQ_LEN, ROPE_DIM), jnp.float32).astype(jnp.bfloat16)
    base_len = jax.random.randint(part_keys[4], (BATCH,), 1, SEQ_LEN)
    pick_rows = jax.random.randint(part_keys[5], (2,), 0, BATCH)
    long_row = pick_rows[0]
    short_row = (long_row + 1 + pick_rows[1] % (BATCH - 1)) % BATCH
    cache_len = base_len.at[long_row].set(SEQ_LEN - 1).at[short_row].set(1)
    inv_freq = 10000.0 ** (-jnp.arange(half_rope, dtype=jnp.float32) / half_rope)
    angles = cache_len.astype(jnp.float32)[:, None] * inv_freq[None, :]
    return dict(
        hidden=hidden,
        ckv_cache=ckv_cache,
        kpe_cache=kpe_cache,
        cache_len=cache_len,
        rope_cos=jnp.cos(angles),
        rope_sin=jnp.sin(angles),
        norm_attn=gain_draw(shared_keys[0], D_MODEL),
        w_dq=weight_draw(shared_keys[1], (D_MODEL, Q_LORA), D_MODEL),
        norm_q=gain_draw(shared_keys[2], Q_LORA),
        w_uq=weight_draw(shared_keys[3], (Q_LORA, HEADS, NOPE_DIM + ROPE_DIM), Q_LORA),
        w_dkv=weight_draw(shared_keys[4], (D_MODEL, KV_LORA + ROPE_DIM), D_MODEL),
        norm_kv=gain_draw(shared_keys[5], KV_LORA),
        w_uk=weight_draw(shared_keys[6], (KV_LORA, HEADS, NOPE_DIM), NOPE_DIM),
        w_uv=weight_draw(shared_keys[7], (KV_LORA, HEADS, V_HEAD), KV_LORA),
        w_out=weight_draw(shared_keys[8], (HEADS, V_HEAD, D_MODEL), HEADS * V_HEAD),
        norm_mlp=gain_draw(shared_keys[9], D_MODEL),
        w_gate=weight_draw(shared_keys[10], (D_MODEL, FF_DIM), D_MODEL),
        w_up=weight_draw(shared_keys[11], (D_MODEL, FF_DIM), D_MODEL),
        w_down=weight_draw(shared_keys[12], (FF_DIM, D_MODEL), FF_DIM),
    )


def rms_norm(values_in, gain_vec):
    floats = values_in.astype(jnp.float32)
    mean_sq = jnp.mean(floats * floats, axis=-1, keepdims=True)
    return floats * lax.rsqrt(mean_sq + EPSILON) * gain_vec.astype(jnp.float32)


def apply_rope(values_in, cos_t, sin_t):
    half_dim = values_in.shape[-1] // 2
    low_half = values_in[..., :half_dim]
    high_half = values_in[..., half_dim:]
    return jnp.concatenate([low_half * cos_t - high_half * sin_t, high_half * cos_t + low_half * sin_t], axis=-1)


def one_request(operands):
    q_abs_row, q_pe_row, ckv_row, kpe_row, len_row, ckv_new_row, kpe_new_row = operands
    ckv_float = ckv_row.astype(jnp.float32)
    scores = (jnp.einsum('hl,tl->ht', q_abs_row.astype(jnp.float32), ckv_float)
              + jnp.einsum('hr,tr->ht', q_pe_row.astype(jnp.float32), kpe_row.astype(jnp.float32))) * SCORE_SCALE
    scores = jnp.where(jnp.arange(SEQ_LEN)[None, :] < len_row, scores, -jnp.inf)
    score_new = (jnp.dot(q_abs_row.astype(jnp.float32), ckv_new_row.astype(jnp.float32))
                 + jnp.dot(q_pe_row.astype(jnp.float32), kpe_new_row.astype(jnp.float32))) * SCORE_SCALE
    row_max = jnp.maximum(jnp.max(scores, axis=1), score_new)
    exp_cache = jnp.exp(scores - row_max[:, None])
    exp_new = jnp.exp(score_new - row_max)
    norm_sum = jnp.sum(exp_cache, axis=1) + exp_new
    weighted = (jnp.einsum('ht,tl->hl', exp_cache.astype(jnp.bfloat16).astype(jnp.float32), ckv_float)
                + exp_new.astype(jnp.bfloat16).astype(jnp.float32)[:, None] * ckv_new_row.astype(jnp.float32)[None, :])
    return (weighted / norm_sum[:, None]).astype(jnp.bfloat16)


def reference(hidden, ckv_cache, kpe_cache, cache_len, rope_cos, rope_sin, norm_attn, w_dq, norm_q, w_uq, w_dkv, norm_kv, w_uk, w_uv, w_out, norm_mlp, w_gate, w_up, w_down):
    normed = rms_norm(hidden, norm_attn).astype(jnp.bfloat16)
    q_latent = rms_norm(jnp.dot(normed, w_dq, preferred_element_type=jnp.float32), norm_q).astype(jnp.bfloat16)
    q_full = jnp.einsum('bl,lhe->bhe', q_latent.astype(jnp.float32), w_uq.astype(jnp.float32))
    q_nope = q_full[..., :NOPE_DIM].astype(jnp.bfloat16)
    q_pe = apply_rope(q_full[..., NOPE_DIM:], rope_cos[:, None, :], rope_sin[:, None, :]).astype(jnp.bfloat16)
    kv_full = jnp.dot(normed, w_dkv, preferred_element_type=jnp.float32)
    ckv_new = rms_norm(kv_full[:, :KV_LORA], norm_kv).astype(jnp.bfloat16)
    kpe_new = apply_rope(kv_full[:, KV_LORA:], rope_cos, rope_sin).astype(jnp.bfloat16)
    q_abs = jnp.einsum('bhn,lhn->bhl', q_nope.astype(jnp.float32), w_uk.astype(jnp.float32)).astype(jnp.bfloat16)
    lat_out = lax.map(one_request, (q_abs, q_pe, ckv_cache, kpe_cache, cache_len, ckv_new, kpe_new))
    head_out = jnp.einsum('bhl,lhv->bhv', lat_out.astype(jnp.float32), w_uv.astype(jnp.float32)).astype(jnp.bfloat16)
    attn_out = jnp.einsum('bhv,hvd->bd', head_out.astype(jnp.float32), w_out.astype(jnp.float32))
    residual = (hidden.astype(jnp.float32) + attn_out).astype(jnp.bfloat16)
    mlp_in = rms_norm(residual, norm_mlp).astype(jnp.bfloat16)
    gate_val = jnp.dot(mlp_in, w_gate, preferred_element_type=jnp.float32)
    up_val = jnp.dot(mlp_in, w_up, preferred_element_type=jnp.float32)
    act_val = (jax.nn.silu(gate_val) * up_val).astype(jnp.bfloat16)
    mlp_out = jnp.dot(act_val, w_down, preferred_element_type=jnp.float32)
    out_hidden = (residual.astype(jnp.float32) + mlp_out).astype(jnp.bfloat16)
    return (out_hidden, ckv_new, kpe_new)
```

```python
import math
import jax
import jax.numpy as jnp
from jax import lax
from jax.experimental import pallas as pl
from jax.experimental.pallas import tpu as pltpu
from jax.sharding import PartitionSpec as P

EPSILON = 1e-6
MSCALE = 0.1 * math.log(40.0) + 1.0


def rms_norm(values_in, gain_vec):
    floats = values_in.astype(jnp.float32)
    mean_sq = jnp.mean(floats * floats, axis=-1, keepdims=True)
    return floats * lax.rsqrt(mean_sq + EPSILON) * gain_vec


def apply_rope(values_in, cos_t, sin_t):
    half_dim = values_in.shape[-1] // 2
    low_half = values_in[..., :half_dim]
    high_half = values_in[..., half_dim:]
    return jnp.concatenate([low_half * cos_t - high_half * sin_t, high_half * cos_t + low_half * sin_t], axis=-1)


GROUP = 8
Q_DEPTH = 4096
Q_PACK = 2
HEAD_PACK = 4
LANES = 128
VMEM_BYTES = 60 * 1024 * 1024


def lane_ids(shape, axis):
    return lax.broadcasted_iota(jnp.int32, shape, axis)


def q_kernel(cq_ref, cos_ref, sin_ref, wa_ref, wb_ref, oa_ref, ob_ref, spread):
    step = pl.program_id(0)
    rows, depth = cq_ref.shape
    wide = LANES * GROUP

    @pl.when(step == 0)
    def _():
        expand = (lane_ids((LANES, wide), 1) // GROUP == lane_ids((LANES, wide), 0)).astype(jnp.bfloat16)
        mine = lane_ids((rows, wide), 1) % GROUP == lane_ids((rows, wide), 0) % GROUP
        for k in range(depth // LANES):
            part = jnp.dot(cq_ref[:, k * LANES:(k + 1) * LANES], expand, preferred_element_type=jnp.float32)
            spread[:, k * wide:(k + 1) * wide] = jnp.where(mine, part, 0.0).astype(jnp.bfloat16)

    plain = step < pl.num_programs(0) * 2 // 3
    for part in range(Q_PACK):
        acc = jnp.zeros((rows, 2 * LANES), jnp.float32)
        count = Q_DEPTH // GROUP
        for at in range(0, depth, count):
            both = jnp.concatenate([wa_ref[at:at + count, part * GROUP:(part + 1) * GROUP, :].reshape(Q_DEPTH, LANES),
                                    wb_ref[at:at + count, part * GROUP:(part + 1) * GROUP, :].reshape(Q_DEPTH, LANES)], axis=1)
            acc = acc + jnp.dot(spread[:, at * GROUP:at * GROUP + Q_DEPTH], both, preferred_element_type=jnp.float32)
        low = acc[:, :LANES]
        high = acc[:, LANES:]
        cos_c = cos_ref[part]
        sin_c = sin_ref[part]
        first = jnp.where(plain, low, low * cos_c - high * sin_c)
        second = jnp.where(plain, high, high * cos_c + low * sin_c)
        batch = rows // GROUP
        oa_ref[:, part * GROUP:(part + 1) * GROUP, :] = first.reshape(batch, GROUP, LANES).astype(jnp.bfloat16)
        ob_ref[:, part * GROUP:(part + 1) * GROUP, :] = second.reshape(batch, GROUP, LANES).astype(jnp.bfloat16)


def q_project(q_latent, w_uq, rope_cos, rope_sin):
    batch, depth = q_latent.shape
    heads, width = w_uq.shape[1], w_uq.shape[2]
    stored = jnp.transpose(w_uq, (0, 2, 1))
    rows = batch * GROUP
    repeated = jnp.broadcast_to(q_latent[:, None, :], (batch, GROUP, depth)).reshape(rows, depth)
    half = rope_cos.shape[1]
    turns = half // (GROUP * Q_PACK)
    nope = (width - 2 * half) // (2 * GROUP * Q_PACK)
    cos_c = rope_cos.reshape(batch, half // GROUP, GROUP).transpose(1, 0, 2).reshape(half // GROUP, rows, 1)
    sin_c = rope_sin.reshape(batch, half // GROUP, GROUP).transpose(1, 0, 2).reshape(half // GROUP, rows, 1)
    steps = nope + turns

    def first_at(j):
        return (0, jnp.where(j < nope, j, j + nope), 0)

    def second_at(j):
        return (0, jnp.where(j < nope, j + nope, j + nope + turns), 0)

    def turn_at(j):
        return (jnp.maximum(j - nope, 0), 0, 0)

    out_a, out_b = pl.pallas_call(
        q_kernel,
        grid=(steps,),
        in_specs=[pl.BlockSpec((rows, depth), lambda j: (0, 0)),
                  pl.BlockSpec((Q_PACK, rows, 1), turn_at), pl.BlockSpec((Q_PACK, rows, 1), turn_at),
                  pl.BlockSpec((depth, Q_PACK * GROUP, heads), first_at), pl.BlockSpec((depth, Q_PACK * GROUP, heads), second_at)],
        out_specs=[pl.BlockSpec((batch, Q_PACK * GROUP, heads), lambda j: (0, j, 0))] * 2,
        out_shape=[jax.ShapeDtypeStruct((batch, steps * Q_PACK * GROUP, heads), jnp.bfloat16)] * 2,
        scratch_shapes=[pltpu.VMEM((rows, depth * GROUP), jnp.bfloat16)],
        compiler_params=pltpu.CompilerParams(vmem_limit_bytes=VMEM_BYTES),
        cost_estimate=pl.CostEstimate(flops=2 * batch * depth * heads * width, bytes_accessed=2 * depth * heads * width, transcendentals=0),
        name='q_project',
    )(repeated, cos_c, sin_c, stored, stored)
    cut = nope * Q_PACK * GROUP
    q_nope = jnp.concatenate([out_a[:, :cut], out_b[:, :cut]], axis=1).transpose(0, 2, 1)
    q_pe = jnp.concatenate([out_a[:, cut:], out_b[:, cut:]], axis=1).transpose(0, 2, 1)
    return q_nope, q_pe


def absorb_kernel(q_ref, w_ref, o_ref, plain):
    batch, heads, inner = q_ref.shape
    outer = w_ref.shape[0]
    rows = batch * GROUP
    own = lane_ids((rows, inner), 0) % GROUP
    for part in range(heads // GROUP):
        span = slice(part * GROUP, (part + 1) * GROUP)
        plain[part] = w_ref[:, span, :].reshape(outer * GROUP, inner).astype(jnp.float32)
        queries = q_ref[:, span, :].reshape(rows, inner)
        acc = jnp.zeros((rows, outer), jnp.float32)
        for h in range(0, GROUP, 2):
            left = jnp.concatenate([jnp.where(own == h, queries, jnp.zeros_like(queries)),
                                    jnp.where(own == h + 1, queries, jnp.zeros_like(queries))], axis=1)
            right = jnp.concatenate([plain[part, pl.ds(h, outer, stride=GROUP), :].astype(jnp.bfloat16),
                                     plain[part, pl.ds(h + 1, outer, stride=GROUP), :].astype(jnp.bfloat16)], axis=1)
            acc = acc + lax.dot_general(left, right, (((1,), (1,)), ((), ())), preferred_element_type=jnp.float32)
        o_ref[:, span, :] = acc.reshape(batch, GROUP, outer).astype(jnp.bfloat16)


def absorb(q_nope, w_uk):
    batch, heads, inner = q_nope.shape
    outer = w_uk.shape[0]
    return pl.pallas_call(
        absorb_kernel,
        grid=(heads // (HEAD_PACK * GROUP),),
        in_specs=[pl.BlockSpec((batch, HEAD_PACK * GROUP, inner), lambda g: (0, g, 0)),
                  pl.BlockSpec((outer, HEAD_PACK * GROUP, inner), lambda g: (0, g, 0))],
        out_specs=pl.BlockSpec((batch, HEAD_PACK * GROUP, outer), lambda g: (0, g, 0)),
        out_shape=jax.ShapeDtypeStruct((batch, heads, outer), jnp.bfloat16),
        scratch_shapes=[pltpu.VMEM((HEAD_PACK, outer * GROUP, inner), jnp.float32)],
        compiler_params=pltpu.CompilerParams(vmem_limit_bytes=VMEM_BYTES),
        cost_estimate=pl.CostEstimate(flops=2 * batch * heads * inner * outer, bytes_accessed=2 * heads * inner * outer, transcendentals=0),
        name='absorb',
    )(q_nope, w_uk)


def value_kernel(l_ref, w_ref, o_ref, plain, picked):
    batch, heads, outer = l_ref.shape
    inner = w_ref.shape[2]
    rows = batch * GROUP
    own = lane_ids((rows, inner), 0) % GROUP
    for part in range(heads // GROUP):
        span = slice(part * GROUP, (part + 1) * GROUP)
        plain[part] = w_ref[:, span, :].reshape(outer * GROUP, inner).astype(jnp.float32)
        latents = l_ref[:, span, :].reshape(rows, outer)
        acc = jnp.zeros((rows, inner), jnp.float32)
        for h in range(0, GROUP, 2):
            right = jnp.concatenate([plain[part, pl.ds(h, outer, stride=GROUP), :].astype(jnp.bfloat16),
                                     plain[part, pl.ds(h + 1, outer, stride=GROUP), :].astype(jnp.bfloat16)], axis=1)
            both = jnp.dot(latents, right, preferred_element_type=jnp.float32)
            acc = jnp.where(own == h, both[:, :inner], jnp.where(own == h + 1, both[:, inner:], acc))
        picked[part] = acc
        for h in range(GROUP):
            o_ref[:, (part * GROUP + h) * inner:(part * GROUP + h + 1) * inner] = picked[part, pl.ds(h, batch, stride=GROUP), :].astype(jnp.bfloat16)


def value_heads(lat_out, w_uv):
    batch, heads, outer = lat_out.shape
    inner = w_uv.shape[2]
    return pl.pallas_call(
        value_kernel,
        grid=(heads // (HEAD_PACK * GROUP),),
        in_specs=[pl.BlockSpec((batch, HEAD_PACK * GROUP, outer), lambda g: (0, g, 0)),
                  pl.BlockSpec((outer, HEAD_PACK * GROUP, inner), lambda g: (0, g, 0))],
        out_specs=pl.BlockSpec((batch, HEAD_PACK * GROUP * inner), lambda g: (0, g)),
        out_shape=jax.ShapeDtypeStruct((batch, heads * inner), jnp.bfloat16),
        scratch_shapes=[pltpu.VMEM((HEAD_PACK, outer * GROUP, inner), jnp.float32), pltpu.VMEM((HEAD_PACK, batch * GROUP, inner), jnp.float32)],
        compiler_params=pltpu.CompilerParams(vmem_limit_bytes=VMEM_BYTES),
        cost_estimate=pl.CostEstimate(flops=2 * batch * heads * inner * outer, bytes_accessed=2 * heads * inner * outer, transcendentals=0),
        name='value_heads',
    )(lat_out, w_uv)


def out_kernel(o_ref, x_ref, w_ref, r_ref, acc):
    step = pl.program_id(0)

    @pl.when(step == 0)
    def _():
        acc[...] = x_ref[...].astype(jnp.float32)

    acc[...] += jnp.dot(o_ref[...], w_ref[...], preferred_element_type=jnp.float32)

    @pl.when(step == pl.num_programs(0) - 1)
    def _():
        r_ref[...] = acc[...].astype(jnp.bfloat16)


OUT_PARTS = 4
OUT_DEPTH = 4096


def out_columns(head_out, hidden, w_flat, part):
    batch, depth = head_out.shape
    columns = w_flat.shape[1] // OUT_PARTS
    return pl.pallas_call(
        out_kernel,
        grid=(depth // OUT_DEPTH,),
        in_specs=[pl.BlockSpec((batch, OUT_DEPTH), lambda k: (0, k)),
                  pl.BlockSpec((batch, columns), lambda k: (0, part)),
                  pl.BlockSpec((OUT_DEPTH, columns), lambda k: (k, part))],
        out_specs=pl.BlockSpec((batch, columns), lambda k: (0, 0)),
        out_shape=jax.ShapeDtypeStruct((batch, columns), jnp.bfloat16),
        scratch_shapes=[pltpu.VMEM((batch, columns), jnp.float32)],
        compiler_params=pltpu.CompilerParams(vmem_limit_bytes=VMEM_BYTES),
        cost_estimate=pl.CostEstimate(flops=2 * batch * depth * columns * 16, bytes_accessed=2 * depth * columns, transcendentals=0),
        name='out_columns',
    )(head_out, hidden, w_flat)


def attention_rows(hidden, ckv_cache, kpe_cache, cache_len, rope_cos, rope_sin, norm_attn, w_dq, norm_q, w_uq, w_dkv, norm_kv, w_uk, w_uv, w_out):
    value_a7 = w_uk.shape[0]
    score_scale = MSCALE * MSCALE / math.sqrt(w_uq.shape[2])
    normed = rms_norm(hidden, norm_attn).astype(jnp.bfloat16)
    q_latent = rms_norm(jnp.dot(normed, w_dq, preferred_element_type=jnp.float32), norm_q).astype(jnp.bfloat16)
    q_nope, q_pe = q_project(q_latent, w_uq, rope_cos, rope_sin)
    kv_full = jnp.dot(normed, w_dkv, preferred_element_type=jnp.float32)
    ckv_new = rms_norm(kv_full[:, :value_a7], norm_kv).astype(jnp.bfloat16)
    kpe_new = apply_rope(kv_full[:, value_a7:], rope_cos, rope_sin).astype(jnp.bfloat16)
    q_abs = absorb(q_nope, w_uk)
    scores = (jnp.einsum('bhl,btl->bht', q_abs, ckv_cache, preferred_element_type=jnp.float32)
              + jnp.einsum('bhr,btr->bht', q_pe, kpe_cache, preferred_element_type=jnp.float32)) * score_scale
    positions = jnp.arange(ckv_cache.shape[1])
    scores = jnp.where(positions[None, None, :] < cache_len[:, None, None], scores, -jnp.inf)
    score_new = (jnp.einsum('bhl,bl->bh', q_abs, ckv_new, preferred_element_type=jnp.float32)
                 + jnp.einsum('bhr,br->bh', q_pe, kpe_new, preferred_element_type=jnp.float32)) * score_scale
    row_max = jnp.maximum(jnp.max(scores, axis=-1), score_new)
    exp_cache = jnp.exp(scores - row_max[..., None])
    exp_new = jnp.exp(score_new - row_max)
    norm_sum = jnp.sum(exp_cache, axis=-1) + exp_new
    weighted = (jnp.einsum('bht,btl->bhl', exp_cache.astype(jnp.bfloat16), ckv_cache, preferred_element_type=jnp.float32)
                + exp_new.astype(jnp.bfloat16).astype(jnp.float32)[..., None] * ckv_new.astype(jnp.float32)[:, None, :])
    lat_out = (weighted / norm_sum[..., None]).astype(jnp.bfloat16)
    head_out = value_heads(lat_out, w_uv)
    w_flat = w_out.reshape(w_out.shape[0] * w_out.shape[1], w_out.shape[2])
    parts = [out_columns(head_out, hidden, w_flat, part) for part in range(OUT_PARTS)]
    return parts, ckv_new, kpe_new


def solution(mesh):
    row_spec = P(('rep', 'dp'), None)
    cube_spec = P(('rep', 'dp'), None, None)
    full_spec = P()
    in_specs = (row_spec, cube_spec, cube_spec, P(('rep', 'dp')), row_spec, row_spec,
                full_spec, full_spec, full_spec, full_spec, full_spec, full_spec, full_spec, full_spec, full_spec, full_spec,
                P(None, 'dp'), P(None, 'dp'), P('dp', None))

    def local_step(hidden, ckv_cache, kpe_cache, cache_len, rope_cos, rope_sin, norm_attn, w_dq, norm_q, w_uq, w_dkv, norm_kv, w_uk, w_uv, w_out, norm_mlp, w_gate, w_up, w_down):
        parts, ckv_new, kpe_new = attention_rows(hidden, ckv_cache, kpe_cache, cache_len, rope_cos, rope_sin, norm_attn, w_dq, norm_q, w_uq, w_dkv, norm_kv, w_uk, w_uv, w_out)
        gathered = [lax.all_gather(part, 'dp', axis=0, tiled=True) for part in parts]
        residual = jnp.concatenate(parts, axis=1)
        group_in = rms_norm(jnp.concatenate(gathered, axis=1), norm_mlp).astype(jnp.bfloat16)
        gate_val = jnp.dot(group_in, w_gate, preferred_element_type=jnp.float32)
        up_val = jnp.dot(group_in, w_up, preferred_element_type=jnp.float32)
        act_val = (jax.nn.silu(gate_val) * up_val).astype(jnp.bfloat16)
        partial_sum = jnp.dot(act_val, w_down, preferred_element_type=jnp.float32)
        mlp_rows = lax.psum_scatter(partial_sum, 'dp', scatter_dimension=0, tiled=True)
        out_hidden = (residual.astype(jnp.float32) + mlp_rows).astype(jnp.bfloat16)
        return out_hidden, ckv_new, kpe_new

    return jax.shard_map(local_step, mesh=mesh, in_specs=in_specs, out_specs=(row_spec, row_spec, row_spec), check_vma=False)
```

```python
import functools
import math
import jax
import jax.numpy as jnp
from jax import lax
from jax.experimental import pallas as pl
from jax.experimental.pallas import tpu as pltpu
from jax.sharding import PartitionSpec as P

EPSILON = 1e-6
MSCALE = 0.1 * math.log(40.0) + 1.0


def rms_norm(values_in, gain_vec):
    floats = values_in.astype(jnp.float32)
    mean_sq = jnp.mean(floats * floats, axis=-1, keepdims=True)
    return floats * lax.rsqrt(mean_sq + EPSILON) * gain_vec


def apply_rope(values_in, cos_t, sin_t):
    half_dim = values_in.shape[-1] // 2
    low_half = values_in[..., :half_dim]
    high_half = values_in[..., half_dim:]
    return jnp.concatenate([low_half * cos_t - high_half * sin_t, high_half * cos_t + low_half * sin_t], axis=-1)


GROUP = 8
Q_DEPTH = 4096
Q_PACK = 2
HEAD_PACK = 4
LANES = 128
VMEM_BYTES = 60 * 1024 * 1024


def lane_ids(shape, axis):
    return lax.broadcasted_iota(jnp.int32, shape, axis)


def q_kernel(cq_ref, cos_ref, sin_ref, wa_ref, wb_ref, oa_ref, ob_ref, spread):
    step = pl.program_id(0)
    rows, depth = cq_ref.shape
    wide = LANES * GROUP

    @pl.when(step == 0)
    def _():
        expand = (lane_ids((LANES, wide), 1) // GROUP == lane_ids((LANES, wide), 0)).astype(jnp.bfloat16)
        mine = lane_ids((rows, wide), 1) % GROUP == lane_ids((rows, wide), 0) % GROUP
        for k in range(depth // LANES):
            part = jnp.dot(cq_ref[:, k * LANES:(k + 1) * LANES], expand, preferred_element_type=jnp.float32)
            spread[:, k * wide:(k + 1) * wide] = jnp.where(mine, part, 0.0).astype(jnp.bfloat16)

    plain = step < pl.num_programs(0) * 2 // 3
    for part in range(Q_PACK):
        acc = jnp.zeros((rows, 2 * LANES), jnp.float32)
        count = Q_DEPTH // GROUP
        for at in range(0, depth, count):
            both = jnp.concatenate([wa_ref[at:at + count, part * GROUP:(part + 1) * GROUP, :].reshape(Q_DEPTH, LANES),
                                    wb_ref[at:at + count, part * GROUP:(part + 1) * GROUP, :].reshape(Q_DEPTH, LANES)], axis=1)
            acc = acc + jnp.dot(spread[:, at * GROUP:at * GROUP + Q_DEPTH], both, preferred_element_type=jnp.float32)
        low = acc[:, :LANES]
        high = acc[:, LANES:]
        cos_c = cos_ref[part]
        sin_c = sin_ref[part]
        first = jnp.where(plain, low, low * cos_c - high * sin_c)
        second = jnp.where(plain, high, high * cos_c + low * sin_c)
        batch = rows // GROUP
        oa_ref[:, part * GROUP:(part + 1) * GROUP, :] = first.reshape(batch, GROUP, LANES).astype(jnp.bfloat16)
        ob_ref[:, part * GROUP:(part + 1) * GROUP, :] = second.reshape(batch, GROUP, LANES).astype(jnp.bfloat16)


def q_project(q_latent, w_uq, rope_cos, rope_sin):
    batch, depth = q_latent.shape
    heads, width = w_uq.shape[1], w_uq.shape[2]
    stored = jnp.transpose(w_uq, (0, 2, 1))
    rows = batch * GROUP
    repeated = jnp.broadcast_to(q_latent[:, None, :], (batch, GROUP, depth)).reshape(rows, depth)
    half = rope_cos.shape[1]
    turns = half // (GROUP * Q_PACK)
    nope = (width - 2 * half) // (2 * GROUP * Q_PACK)
    cos_c = rope_cos.reshape(batch, half // GROUP, GROUP).transpose(1, 0, 2).reshape(half // GROUP, rows, 1)
    sin_c = rope_sin.reshape(batch, half // GROUP, GROUP).transpose(1, 0, 2).reshape(half // GROUP, rows, 1)
    steps = nope + turns

    def first_at(j):
        return (0, jnp.where(j < nope, j, j + nope), 0)

    def second_at(j):
        return (0, jnp.where(j < nope, j + nope, j + nope + turns), 0)

    def turn_at(j):
        return (jnp.maximum(j - nope, 0), 0, 0)

    out_a, out_b = pl.pallas_call(
        q_kernel,
        grid=(steps,),
        in_specs=[pl.BlockSpec((rows, depth), lambda j: (0, 0)),
                  pl.BlockSpec((Q_PACK, rows, 1), turn_at), pl.BlockSpec((Q_PACK, rows, 1), turn_at),
                  pl.BlockSpec((depth, Q_PACK * GROUP, heads), first_at), pl.BlockSpec((depth, Q_PACK * GROUP, heads), second_at)],
        out_specs=[pl.BlockSpec((batch, Q_PACK * GROUP, heads), lambda j: (0, j, 0))] * 2,
        out_shape=[jax.ShapeDtypeStruct((batch, steps * Q_PACK * GROUP, heads), jnp.bfloat16)] * 2,
        scratch_shapes=[pltpu.VMEM((rows, depth * GROUP), jnp.bfloat16)],
        compiler_params=pltpu.CompilerParams(vmem_limit_bytes=VMEM_BYTES),
        cost_estimate=pl.CostEstimate(flops=2 * batch * depth * heads * width, bytes_accessed=2 * depth * heads * width, transcendentals=0),
        name='q_project',
    )(repeated, cos_c, sin_c, stored, stored)
    cut = nope * Q_PACK * GROUP
    q_nope = jnp.concatenate([out_a[:, :cut], out_b[:, :cut]], axis=1).transpose(0, 2, 1)
    q_pe = jnp.concatenate([out_a[:, cut:], out_b[:, cut:]], axis=1).transpose(0, 2, 1)
    return q_nope, q_pe


def absorb_kernel(q_ref, w_ref, o_ref, plain):
    batch, heads, inner = q_ref.shape
    outer = w_ref.shape[0]
    rows = batch * GROUP
    own = lane_ids((rows, inner), 0) % GROUP
    for part in range(heads // GROUP):
        span = slice(part * GROUP, (part + 1) * GROUP)
        plain[part] = w_ref[:, span, :].reshape(outer * GROUP, inner).astype(jnp.float32)
        queries = q_ref[:, span, :].reshape(rows, inner)
        acc = jnp.zeros((rows, outer), jnp.float32)
        for h in range(0, GROUP, 2):
            left = jnp.concatenate([jnp.where(own == h, queries, jnp.zeros_like(queries)),
                                    jnp.where(own == h + 1, queries, jnp.zeros_like(queries))], axis=1)
            right = jnp.concatenate([plain[part, pl.ds(h, outer, stride=GROUP), :].astype(jnp.bfloat16),
                                     plain[part, pl.ds(h + 1, outer, stride=GROUP), :].astype(jnp.bfloat16)], axis=1)
            acc = acc + lax.dot_general(left, right, (((1,), (1,)), ((), ())), preferred_element_type=jnp.float32)
        o_ref[:, span, :] = acc.reshape(batch, GROUP, outer).astype(jnp.bfloat16)


def absorb(q_nope, w_uk):
    batch, heads, inner = q_nope.shape
    outer = w_uk.shape[0]
    return pl.pallas_call(
        absorb_kernel,
        grid=(heads // (HEAD_PACK * GROUP),),
        in_specs=[pl.BlockSpec((batch, HEAD_PACK * GROUP, inner), lambda g: (0, g, 0)),
                  pl.BlockSpec((outer, HEAD_PACK * GROUP, inner), lambda g: (0, g, 0))],
        out_specs=pl.BlockSpec((batch, HEAD_PACK * GROUP, outer), lambda g: (0, g, 0)),
        out_shape=jax.ShapeDtypeStruct((batch, heads, outer), jnp.bfloat16),
        scratch_shapes=[pltpu.VMEM((HEAD_PACK, outer * GROUP, inner), jnp.float32)],
        compiler_params=pltpu.CompilerParams(vmem_limit_bytes=VMEM_BYTES),
        cost_estimate=pl.CostEstimate(flops=2 * batch * heads * inner * outer, bytes_accessed=2 * heads * inner * outer, transcendentals=0),
        name='absorb',
    )(q_nope, w_uk)


def value_kernel(l_ref, w_ref, o_ref, plain, picked):
    batch, heads, outer = l_ref.shape
    inner = w_ref.shape[2]
    rows = batch * GROUP
    own = lane_ids((rows, inner), 0) % GROUP
    for part in range(heads // GROUP):
        span = slice(part * GROUP, (part + 1) * GROUP)
        plain[part] = w_ref[:, span, :].reshape(outer * GROUP, inner).astype(jnp.float32)
        latents = l_ref[:, span, :].reshape(rows, outer)
        acc = jnp.zeros((rows, inner), jnp.float32)
        for h in range(0, GROUP, 2):
            right = jnp.concatenate([plain[part, pl.ds(h, outer, stride=GROUP), :].astype(jnp.bfloat16),
                                     plain[part, pl.ds(h + 1, outer, stride=GROUP), :].astype(jnp.bfloat16)], axis=1)
            both = jnp.dot(latents, right, preferred_element_type=jnp.float32)
            acc = jnp.where(own == h, both[:, :inner], jnp.where(own == h + 1, both[:, inner:], acc))
        picked[part] = acc
        for h in range(GROUP):
            o_ref[:, (part * GROUP + h) * inner:(part * GROUP + h + 1) * inner] = picked[part, pl.ds(h, batch, stride=GROUP), :].astype(jnp.bfloat16)


def value_heads(lat_out, w_uv):
    batch, heads, outer = lat_out.shape
    inner = w_uv.shape[2]
    return pl.pallas_call(
        value_kernel,
        grid=(heads // (HEAD_PACK * GROUP),),
        in_specs=[pl.BlockSpec((batch, HEAD_PACK * GROUP, outer), lambda g: (0, g, 0)),
                  pl.BlockSpec((outer, HEAD_PACK * GROUP, inner), lambda g: (0, g, 0))],
        out_specs=pl.BlockSpec((batch, HEAD_PACK * GROUP * inner), lambda g: (0, g)),
        out_shape=jax.ShapeDtypeStruct((batch, heads * inner), jnp.bfloat16),
        scratch_shapes=[pltpu.VMEM((HEAD_PACK, outer * GROUP, inner), jnp.float32), pltpu.VMEM((HEAD_PACK, batch * GROUP, inner), jnp.float32)],
        compiler_params=pltpu.CompilerParams(vmem_limit_bytes=VMEM_BYTES),
        cost_estimate=pl.CostEstimate(flops=2 * batch * heads * inner * outer, bytes_accessed=2 * heads * inner * outer, transcendentals=0),
        name='value_heads',
    )(lat_out, w_uv)


def mlp_kernel(axis, chips, u_ref, r_ref, gate_hbm, up_hbm, down_hbm, o_ref, gate_w, up_w, down_w, rows_in, acts, ring, peer_out, peer_in, contrib, fin_in,
               load_sem, ag_send, ag_recv, pe_send, pe_recv, rs_send, rs_recv, px_send, px_recv, fin_send, fin_recv):
    me = lax.axis_index(axis)
    core = lax.rem(me, 2)
    other = 1 - core
    chip = lax.div(me, 2)
    peer = chip * 2 + other
    ahead = lax.rem(chip + 1, chips) * 2 + core
    behind = lax.rem(chip + chips - 1, chips) * 2 + core
    sides = (ahead, behind)
    half_way = chips // 2
    width = u_ref.shape[-1]
    quarter = width // 4
    tile = 256
    sub_rows = u_ref.shape[1]
    own_rows = 2 * sub_rows
    block_rows = 2 * own_rows
    hidden = gate_w.shape[1]

    loads = [pltpu.make_async_copy(src, dst, load_sem.at[n]) for n, (src, dst) in enumerate(((gate_hbm, gate_w), (up_hbm, up_w), (down_hbm, down_w)))]
    for load in loads:
        load.start()

    barrier = pltpu.get_barrier_semaphore()
    for device in (ahead, behind, peer):
        pl.semaphore_signal(barrier, inc=1, device_id={axis: device}, device_id_type=pl.DeviceIdType.MESH)
    pl.semaphore_wait(barrier, 3)

    def remote(src, dst, send, recv, device):
        return pltpu.make_async_remote_copy(src_ref=src, dst_ref=dst, send_sem=send, recv_sem=recv, device_id={axis: device}, device_id_type=pl.DeviceIdType.MESH)

    def block_at(side, hop):
        return hop if side == 0 else lax.rem(chips - hop, chips)

    def hop_copy(side, hop, sub):
        src = u_ref.at[sub] if isinstance(hop, int) and hop == 1 else rows_in.at[block_at(side, hop - 1), core, sub]
        return remote(src, rows_in.at[block_at(side, hop), core, sub], ag_send.at[side, hop - 1, sub], ag_recv.at[side, hop - 1, sub], sides[side])

    def peer_copy(block):
        src = u_ref if isinstance(block, int) and block == 0 else rows_in.at[block, core]
        return remote(src, rows_in.at[block, core], pe_send.at[block], pe_recv.at[block], peer)

    for sub in range(2):
        for side in range(2):
            hop_copy(side, 1, sub).start()
    peer_copy(0).start()
    rows_in[0, core] = u_ref[...]
    loads[0].wait()
    loads[1].wait()

    def gather_step(hop, carry):
        last = hop == half_way
        for sub in range(2):
            for side in range(2):
                def arrive(side=side, sub=sub):
                    remote(rows_in.at[block_at(side, hop), core, sub], rows_in.at[block_at(side, hop), core, sub], ag_send.at[side, hop - 1, sub], ag_recv.at[side, hop - 1, sub], sides[side]).wait_recv()

                def forward(side=side, sub=sub):
                    hop_copy(side, hop + 1, sub).start()

                if side == sub:
                    arrive()
                    pl.when(jnp.logical_not(last))(forward)
                else:
                    pl.when(jnp.logical_not(last))(arrive)
                    pl.when(hop < half_way - 1)(forward)
        first = hop
        second = jnp.where(last, 0, chips - hop)
        peer_copy(first).start()

        @pl.when(jnp.logical_not(last))
        def _():
            peer_copy(second).start()

        peer_copy(first).wait_recv()
        peer_copy(second).wait_recv()
        for_first = rows_in[first].reshape(block_rows, width)
        for_second = rows_in[second].reshape(block_rows, width)
        both = jnp.concatenate([for_first, for_second], axis=0)

        def columns(n, carry):
            at = pl.ds(pl.multiple_of(n * tile, tile), tile)
            gate = jnp.dot(both, gate_w[:, at], preferred_element_type=jnp.float32)
            up = jnp.dot(both, up_w[:, at], preferred_element_type=jnp.float32)
            act = (jax.nn.silu(gate) * up).astype(jnp.bfloat16)
            acts[first, :, at] = act[:block_rows]
            acts[second, :, at] = act[block_rows:]
            return carry

        lax.fori_loop(0, hidden // tile, columns, 0)
        return carry

    lax.fori_loop(1, half_way + 1, gather_step, 0)
    loads[2].wait()

    def swap_copy(side, step):
        return remote(peer_out.at[side, step], peer_in.at[side, step], px_send.at[side, step], px_recv.at[side, step], peer)

    def ring_copy(side, step, sub):
        return remote(ring.at[side, step, sub], ring.at[side, step + 1, sub], rs_send.at[side, step, sub], rs_recv.at[side, step, sub], sides[side])

    def partial_sums(step):
        blocks = (lax.rem(step + 1, chips), chips - 1 - step)
        acted = [acts[block] for block in blocks]

        def columns(n, carry):
            at = pl.ds(pl.multiple_of(n * tile, tile), tile)
            for side in range(2):
                base = side * 2 * quarter + n * tile
                kept = jnp.dot(acted[side], down_w[:, pl.ds(pl.multiple_of(base + core * quarter, 128), tile)], preferred_element_type=jnp.float32)
                sent = jnp.dot(acted[side], down_w[:, pl.ds(pl.multiple_of(base + other * quarter, 128), tile)], preferred_element_type=jnp.float32)
                contrib[side, :, :, at] = kept.reshape(2, own_rows, tile)
                peer_out[side, step, :, :, at] = sent.reshape(2, own_rows, tile)
            return carry

        lax.fori_loop(0, quarter // tile, columns, 0)
        for side in range(2):
            swap_copy(side, step).start()

    partial_sums(0)
    for side in range(2):
        swap_copy(side, 0).wait_recv()
        for sub in range(2):
            ring[side, 0, sub] = contrib[side, sub] + peer_in[side, 0, sub]
            ring_copy(side, 0, sub).start()

    def reduce_step(step, carry):
        partial_sums(step)
        for side in range(2):
            swap_copy(side, step).wait_recv()
        for sub in range(2):
            for side in range(2):
                ring_copy(side, step - 1, sub).wait_recv()
                ring[side, step, sub] = ring[side, step, sub] + (contrib[side, sub] + peer_in[side, step, sub])
                ring_copy(side, step, sub).start()
        return carry

    lax.fori_loop(1, chips - 1, reduce_step, 0)
    final = chips - 1
    partial_sums(final)
    for side in range(2):
        swap_copy(side, final).wait_recv()
    for sub in range(2):
        for side in range(2):
            ring_copy(side, final - 1, sub).wait_recv()
            ring[side, final, sub] = ring[side, final, sub] + (contrib[side, sub] + peer_in[side, final, sub])

    def fin_copy(side):
        return remote(ring.at[side, final, other], fin_in.at[side], fin_send.at[side], fin_recv.at[side], peer)

    for side in range(2):
        fin_copy(side).start()
    for side in range(2):
        mine = pl.ds(pl.multiple_of((2 * side + core) * quarter, 128), quarter)
        o_ref[:, mine] = (r_ref[:, mine].astype(jnp.float32) + ring[side, final, core]).astype(jnp.bfloat16)
    for side in range(2):
        theirs = pl.ds(pl.multiple_of((2 * side + other) * quarter, 128), quarter)
        fin_copy(side).wait_recv()
        o_ref[:, theirs] = (r_ref[:, theirs].astype(jnp.float32) + fin_in[side]).astype(jnp.bfloat16)

    for side in range(2):
        fin_copy(side).wait_send()
        for sub in range(2):
            for hop in range(1, half_way + 1):
                if hop < half_way or side == sub:
                    hop_copy(side, hop, sub).wait_send()

    def drain(step, carry):
        for side in range(2):
            swap_copy(side, step).wait_send()
            for sub in range(2):
                pl.when(step < final)(lambda side=side, sub=sub: ring_copy(side, step, sub).wait_send())
        peer_copy(step).wait_send()
        return carry

    lax.fori_loop(0, chips, drain, 0)


def mlp_group(axis, devices, mlp_in, residual, w_gate, w_up, w_down):
    chips = devices // 2
    rows, width = mlp_in.shape
    hidden = w_gate.shape[1]
    quarter = width // 4
    dma = pltpu.SemaphoreType.DMA
    any_spec = pl.BlockSpec(memory_space=pl.ANY)
    vmem_spec = pl.BlockSpec(memory_space=pltpu.VMEM)
    return pl.pallas_call(
        functools.partial(mlp_kernel, axis, chips),
        in_specs=[vmem_spec, vmem_spec, any_spec, any_spec, any_spec],
        out_specs=vmem_spec,
        out_shape=jax.ShapeDtypeStruct((rows, width), jnp.bfloat16),
        scratch_shapes=[pltpu.VMEM((width, hidden), jnp.bfloat16), pltpu.VMEM((width, hidden), jnp.bfloat16), pltpu.VMEM((hidden, width), jnp.bfloat16),
                        pltpu.VMEM((chips, 2, 2, rows // 2, width), jnp.bfloat16), pltpu.VMEM((chips, 2 * rows, hidden), jnp.bfloat16),
                        pltpu.VMEM((2, chips, 2, rows, quarter), jnp.float32), pltpu.VMEM((2, chips, 2, rows, quarter), jnp.float32),
                        pltpu.VMEM((2, chips, 2, rows, quarter), jnp.float32), pltpu.VMEM((2, 2, rows, quarter), jnp.float32), pltpu.VMEM((2, rows, quarter), jnp.float32),
                        dma((3,)), dma((2, chips // 2, 2)), dma((2, chips // 2, 2)), dma((chips,)), dma((chips,)),
                        dma((2, chips, 2)), dma((2, chips, 2)), dma((2, chips)), dma((2, chips)), dma((2,)), dma((2,))],
        compiler_params=pltpu.CompilerParams(collective_id=0, has_side_effects=True, vmem_limit_bytes=VMEM_BYTES),
        name='mlp_group',
    )(mlp_in.reshape(2, rows // 2, width), residual, w_gate, w_up, w_down)


def attention_rows(hidden, ckv_cache, kpe_cache, cache_len, rope_cos, rope_sin, norm_attn, w_dq, norm_q, w_uq, w_dkv, norm_kv, w_uk, w_uv, w_out):
    value_a7 = w_uk.shape[0]
    score_scale = MSCALE * MSCALE / math.sqrt(w_uq.shape[2])
    normed = rms_norm(hidden, norm_attn).astype(jnp.bfloat16)
    q_latent = rms_norm(jnp.dot(normed, w_dq, preferred_element_type=jnp.float32), norm_q).astype(jnp.bfloat16)
    q_nope, q_pe = q_project(q_latent, w_uq, rope_cos, rope_sin)
    kv_full = jnp.dot(normed, w_dkv, preferred_element_type=jnp.float32)
    ckv_new = rms_norm(kv_full[:, :value_a7], norm_kv).astype(jnp.bfloat16)
    kpe_new = apply_rope(kv_full[:, value_a7:], rope_cos, rope_sin).astype(jnp.bfloat16)
    q_abs = absorb(q_nope, w_uk)
    scores = (jnp.einsum('bhl,btl->bht', q_abs, ckv_cache, preferred_element_type=jnp.float32)
              + jnp.einsum('bhr,btr->bht', q_pe, kpe_cache, preferred_element_type=jnp.float32)) * score_scale
    positions = jnp.arange(ckv_cache.shape[1])
    scores = jnp.where(positions[None, None, :] < cache_len[:, None, None], scores, -jnp.inf)
    score_new = (jnp.einsum('bhl,bl->bh', q_abs, ckv_new, preferred_element_type=jnp.float32)
                 + jnp.einsum('bhr,br->bh', q_pe, kpe_new, preferred_element_type=jnp.float32)) * score_scale
    row_max = jnp.maximum(jnp.max(scores, axis=-1), score_new)
    exp_cache = jnp.exp(scores - row_max[..., None])
    exp_new = jnp.exp(score_new - row_max)
    norm_sum = jnp.sum(exp_cache, axis=-1) + exp_new
    weighted = (jnp.einsum('bht,btl->bhl', exp_cache.astype(jnp.bfloat16), ckv_cache, preferred_element_type=jnp.float32)
                + exp_new.astype(jnp.bfloat16).astype(jnp.float32)[..., None] * ckv_new.astype(jnp.float32)[:, None, :])
    lat_out = (weighted / norm_sum[..., None]).astype(jnp.bfloat16)
    head_out = value_heads(lat_out, w_uv)
    attn_out = jnp.dot(head_out, w_out.reshape(w_out.shape[0] * w_out.shape[1], w_out.shape[2]), preferred_element_type=jnp.float32)
    residual = (hidden.astype(jnp.float32) + attn_out).astype(jnp.bfloat16)
    return residual, ckv_new, kpe_new


def solution(mesh):
    row_spec = P(('rep', 'dp'), None)
    cube_spec = P(('rep', 'dp'), None, None)
    full_spec = P()
    in_specs = (row_spec, cube_spec, cube_spec, P(('rep', 'dp')), row_spec, row_spec,
                full_spec, full_spec, full_spec, full_spec, full_spec, full_spec, full_spec, full_spec, full_spec, full_spec,
                P(None, 'dp'), P(None, 'dp'), P('dp', None))

    def local_step(hidden, ckv_cache, kpe_cache, cache_len, rope_cos, rope_sin, norm_attn, w_dq, norm_q, w_uq, w_dkv, norm_kv, w_uk, w_uv, w_out, norm_mlp, w_gate, w_up, w_down):
        residual, ckv_new, kpe_new = attention_rows(hidden, ckv_cache, kpe_cache, cache_len, rope_cos, rope_sin, norm_attn, w_dq, norm_q, w_uq, w_dkv, norm_kv, w_uk, w_uv, w_out)
        mlp_in = rms_norm(residual, norm_mlp).astype(jnp.bfloat16)
        out_hidden = mlp_group('dp', mesh.shape['dp'], mlp_in, residual, w_gate, w_up, w_down)
        return out_hidden, ckv_new, kpe_new

    return jax.shard_map(local_step, mesh=mesh, in_specs=in_specs, out_specs=(row_spec, row_spec, row_spec), check_vma=False)
```

```python
import functools
import math
import jax
import jax.numpy as jnp
from jax import lax
from jax.experimental import pallas as pl
from jax.experimental.pallas import tpu as pltpu
from jax.sharding import PartitionSpec as P

EPSILON = 1e-6
MSCALE = 0.1 * math.log(40.0) + 1.0


def rms_norm(values_in, gain_vec):
    floats = values_in.astype(jnp.float32)
    mean_sq = jnp.mean(floats * floats, axis=-1, keepdims=True)
    return floats * lax.rsqrt(mean_sq + EPSILON) * gain_vec


def apply_rope(values_in, cos_t, sin_t):
    half_dim = values_in.shape[-1] // 2
    low_half = values_in[..., :half_dim]
    high_half = values_in[..., half_dim:]
    return jnp.concatenate([low_half * cos_t - high_half * sin_t, high_half * cos_t + low_half * sin_t], axis=-1)


GROUP = 8
Q_DEPTH = 4096
Q_PACK = 2
HEAD_PACK = 4
LANES = 128
VMEM_BYTES = 60 * 1024 * 1024


def lane_ids(shape, axis):
    return lax.broadcasted_iota(jnp.int32, shape, axis)


def q_kernel(cq_ref, cos_ref, sin_ref, wa_ref, wb_ref, oa_ref, ob_ref, spread):
    step = pl.program_id(0)
    rows, depth = cq_ref.shape
    wide = LANES * GROUP

    @pl.when(step == 0)
    def _():
        expand = (lane_ids((LANES, wide), 1) // GROUP == lane_ids((LANES, wide), 0)).astype(jnp.bfloat16)
        mine = lane_ids((rows, wide), 1) % GROUP == lane_ids((rows, wide), 0) % GROUP
        for k in range(depth // LANES):
            part = jnp.dot(cq_ref[:, k * LANES:(k + 1) * LANES], expand, preferred_element_type=jnp.float32)
            spread[:, k * wide:(k + 1) * wide] = jnp.where(mine, part, 0.0).astype(jnp.bfloat16)

    plain = step < pl.num_programs(0) * 2 // 3
    for part in range(Q_PACK):
        acc = jnp.zeros((rows, 2 * LANES), jnp.float32)
        count = Q_DEPTH // GROUP
        for at in range(0, depth, count):
            both = jnp.concatenate([wa_ref[at:at + count, part * GROUP:(part + 1) * GROUP, :].reshape(Q_DEPTH, LANES),
                                    wb_ref[at:at + count, part * GROUP:(part + 1) * GROUP, :].reshape(Q_DEPTH, LANES)], axis=1)
            acc = acc + jnp.dot(spread[:, at * GROUP:at * GROUP + Q_DEPTH], both, preferred_element_type=jnp.float32)
        low = acc[:, :LANES]
        high = acc[:, LANES:]
        cos_c = cos_ref[part]
        sin_c = sin_ref[part]
        first = jnp.where(plain, low, low * cos_c - high * sin_c)
        second = jnp.where(plain, high, high * cos_c + low * sin_c)
        batch = rows // GROUP
        oa_ref[:, part * GROUP:(part + 1) * GROUP, :] = first.reshape(batch, GROUP, LANES).astype(jnp.bfloat16)
        ob_ref[:, part * GROUP:(part + 1) * GROUP, :] = second.reshape(batch, GROUP, LANES).astype(jnp.bfloat16)


def q_project(q_latent, w_uq, rope_cos, rope_sin):
    batch, depth = q_latent.shape
    heads, width = w_uq.shape[1], w_uq.shape[2]
    stored = jnp.transpose(w_uq, (0, 2, 1))
    rows = batch * GROUP
    repeated = jnp.broadcast_to(q_latent[:, None, :], (batch, GROUP, depth)).reshape(rows, depth)
    half = rope_cos.shape[1]
    turns = half // (GROUP * Q_PACK)
    nope = (width - 2 * half) // (2 * GROUP * Q_PACK)
    cos_c = rope_cos.reshape(batch, half // GROUP, GROUP).transpose(1, 0, 2).reshape(half // GROUP, rows, 1)
    sin_c = rope_sin.reshape(batch, half // GROUP, GROUP).transpose(1, 0, 2).reshape(half // GROUP, rows, 1)
    steps = nope + turns

    def first_at(j):
        return (0, jnp.where(j < nope, j, j + nope), 0)

    def second_at(j):
        return (0, jnp.where(j < nope, j + nope, j + nope + turns), 0)

    def turn_at(j):
        return (jnp.maximum(j - nope, 0), 0, 0)

    out_a, out_b = pl.pallas_call(
        q_kernel,
        grid=(steps,),
        in_specs=[pl.BlockSpec((rows, depth), lambda j: (0, 0)),
                  pl.BlockSpec((Q_PACK, rows, 1), turn_at), pl.BlockSpec((Q_PACK, rows, 1), turn_at),
                  pl.BlockSpec((depth, Q_PACK * GROUP, heads), first_at), pl.BlockSpec((depth, Q_PACK * GROUP, heads), second_at)],
        out_specs=[pl.BlockSpec((batch, Q_PACK * GROUP, heads), lambda j: (0, j, 0))] * 2,
        out_shape=[jax.ShapeDtypeStruct((batch, steps * Q_PACK * GROUP, heads), jnp.bfloat16)] * 2,
        scratch_shapes=[pltpu.VMEM((rows, depth * GROUP), jnp.bfloat16)],
        compiler_params=pltpu.CompilerParams(vmem_limit_bytes=VMEM_BYTES),
        cost_estimate=pl.CostEstimate(flops=2 * batch * depth * heads * width, bytes_accessed=2 * depth * heads * width, transcendentals=0),
        name='q_project',
    )(repeated, cos_c, sin_c, stored, stored)
    cut = nope * Q_PACK * GROUP
    q_nope = jnp.concatenate([out_a[:, :cut], out_b[:, :cut]], axis=1).transpose(0, 2, 1)
    q_pe = jnp.concatenate([out_a[:, cut:], out_b[:, cut:]], axis=1).transpose(0, 2, 1)
    return q_nope, q_pe


def absorb_kernel(q_ref, w_ref, o_ref, plain):
    batch, heads, inner = q_ref.shape
    outer = w_ref.shape[0]
    rows = batch * GROUP
    own = lane_ids((rows, inner), 0) % GROUP
    for part in range(heads // GROUP):
        span = slice(part * GROUP, (part + 1) * GROUP)
        plain[part] = w_ref[:, span, :].reshape(outer * GROUP, inner).astype(jnp.float32)
        queries = q_ref[:, span, :].reshape(rows, inner)
        acc = jnp.zeros((rows, outer), jnp.float32)
        for h in range(0, GROUP, 2):
            left = jnp.concatenate([jnp.where(own == h, queries, jnp.zeros_like(queries)),
                                    jnp.where(own == h + 1, queries, jnp.zeros_like(queries))], axis=1)
            right = jnp.concatenate([plain[part, pl.ds(h, outer, stride=GROUP), :].astype(jnp.bfloat16),
                                     plain[part, pl.ds(h + 1, outer, stride=GROUP), :].astype(jnp.bfloat16)], axis=1)
            acc = acc + lax.dot_general(left, right, (((1,), (1,)), ((), ())), preferred_element_type=jnp.float32)
        o_ref[:, span, :] = acc.reshape(batch, GROUP, outer).astype(jnp.bfloat16)


def absorb(q_nope, w_uk):
    batch, heads, inner = q_nope.shape
    outer = w_uk.shape[0]
    return pl.pallas_call(
        absorb_kernel,
        grid=(heads // (HEAD_PACK * GROUP),),
        in_specs=[pl.BlockSpec((batch, HEAD_PACK * GROUP, inner), lambda g: (0, g, 0)),
                  pl.BlockSpec((outer, HEAD_PACK * GROUP, inner), lambda g: (0, g, 0))],
        out_specs=pl.BlockSpec((batch, HEAD_PACK * GROUP, outer), lambda g: (0, g, 0)),
        out_shape=jax.ShapeDtypeStruct((batch, heads, outer), jnp.bfloat16),
        scratch_shapes=[pltpu.VMEM((HEAD_PACK, outer * GROUP, inner), jnp.float32)],
        compiler_params=pltpu.CompilerParams(vmem_limit_bytes=VMEM_BYTES),
        cost_estimate=pl.CostEstimate(flops=2 * batch * heads * inner * outer, bytes_accessed=2 * heads * inner * outer, transcendentals=0),
        name='absorb',
    )(q_nope, w_uk)


def value_kernel(l_ref, w_ref, o_ref, plain, picked):
    batch, heads, outer = l_ref.shape
    inner = w_ref.shape[2]
    rows = batch * GROUP
    own = lane_ids((rows, inner), 0) % GROUP
    for part in range(heads // GROUP):
        span = slice(part * GROUP, (part + 1) * GROUP)
        plain[part] = w_ref[:, span, :].reshape(outer * GROUP, inner).astype(jnp.float32)
        latents = l_ref[:, span, :].reshape(rows, outer)
        acc = jnp.zeros((rows, inner), jnp.float32)
        for h in range(0, GROUP, 2):
            right = jnp.concatenate([plain[part, pl.ds(h, outer, stride=GROUP), :].astype(jnp.bfloat16),
                                     plain[part, pl.ds(h + 1, outer, stride=GROUP), :].astype(jnp.bfloat16)], axis=1)
            both = jnp.dot(latents, right, preferred_element_type=jnp.float32)
            acc = jnp.where(own == h, both[:, :inner], jnp.where(own == h + 1, both[:, inner:], acc))
        picked[part] = acc
        for h in range(GROUP):
            o_ref[:, (part * GROUP + h) * inner:(part * GROUP + h + 1) * inner] = picked[part, pl.ds(h, batch, stride=GROUP), :].astype(jnp.bfloat16)


def value_heads(lat_out, w_uv):
    batch, heads, outer = lat_out.shape
    inner = w_uv.shape[2]
    return pl.pallas_call(
        value_kernel,
        grid=(heads // (HEAD_PACK * GROUP),),
        in_specs=[pl.BlockSpec((batch, HEAD_PACK * GROUP, outer), lambda g: (0, g, 0)),
                  pl.BlockSpec((outer, HEAD_PACK * GROUP, inner), lambda g: (0, g, 0))],
        out_specs=pl.BlockSpec((batch, HEAD_PACK * GROUP * inner), lambda g: (0, g)),
        out_shape=jax.ShapeDtypeStruct((batch, heads * inner), jnp.bfloat16),
        scratch_shapes=[pltpu.VMEM((HEAD_PACK, outer * GROUP, inner), jnp.float32), pltpu.VMEM((HEAD_PACK, batch * GROUP, inner), jnp.float32)],
        compiler_params=pltpu.CompilerParams(vmem_limit_bytes=VMEM_BYTES),
        cost_estimate=pl.CostEstimate(flops=2 * batch * heads * inner * outer, bytes_accessed=2 * heads * inner * outer, transcendentals=0),
        name='value_heads',
    )(lat_out, w_uv)


def mlp_kernel(axis, chips, u_ref, r_ref, gate_hbm, up_hbm, down_hbm, o_ref, gate_w, up_w, down_w, rows_in, acts, ring, peer_out, peer_in, contrib, fin_in,
               load_sem, ag_send, ag_recv, pe_send, pe_recv, rs_send, rs_recv, px_send, px_recv, fin_send, fin_recv):
    me = lax.axis_index(axis)
    core = lax.rem(me, 2)
    other = 1 - core
    chip = lax.div(me, 2)
    peer = chip * 2 + other
    ahead = lax.rem(chip + 1, chips) * 2 + core
    behind = lax.rem(chip + chips - 1, chips) * 2 + core
    sides = (ahead, behind)
    half_way = chips // 2
    width = u_ref.shape[-1]
    quarter = width // 4
    tile = 256
    sub_rows = u_ref.shape[1]
    own_rows = 2 * sub_rows
    block_rows = 2 * own_rows
    hidden = gate_w.shape[1]

    loads = [pltpu.make_async_copy(src, dst, load_sem.at[n]) for n, (src, dst) in enumerate(((gate_hbm, gate_w), (up_hbm, up_w), (down_hbm, down_w)))]
    for load in loads:
        load.start()

    barrier = pltpu.get_barrier_semaphore()
    for device in (ahead, behind, peer):
        pl.semaphore_signal(barrier, inc=1, device_id={axis: device}, device_id_type=pl.DeviceIdType.MESH)
    pl.semaphore_wait(barrier, 3)

    def remote(src, dst, send, recv, device):
        return pltpu.make_async_remote_copy(src_ref=src, dst_ref=dst, send_sem=send, recv_sem=recv, device_id={axis: device}, device_id_type=pl.DeviceIdType.MESH)

    def block_at(side, hop):
        return hop if side == 0 else lax.rem(chips - hop, chips)

    def hop_copy(side, hop, sub):
        src = u_ref.at[sub] if isinstance(hop, int) and hop == 1 else rows_in.at[block_at(side, hop - 1), core, sub]
        return remote(src, rows_in.at[block_at(side, hop), core, sub], ag_send.at[side, hop - 1, sub], ag_recv.at[side, hop - 1, sub], sides[side])

    def peer_copy(block):
        src = u_ref if isinstance(block, int) and block == 0 else rows_in.at[block, core]
        return remote(src, rows_in.at[block, core], pe_send.at[block], pe_recv.at[block], peer)

    for sub in range(2):
        for side in range(2):
            hop_copy(side, 1, sub).start()
    peer_copy(0).start()
    rows_in[0, core] = u_ref[...]
    for load in loads:
        load.wait()

    final = chips - 1

    def swap_copy(side, step):
        return remote(peer_out.at[side, step], peer_in.at[side, step], px_send.at[side, step], px_recv.at[side, step], peer)

    def ring_copy(side, step, sub):
        return remote(ring.at[side, step, sub], ring.at[side, step + 1, sub], rs_send.at[side, step, sub], rs_recv.at[side, step, sub], sides[side])

    def partial_sums(step):
        blocks = (lax.rem(step + 1, chips), chips - 1 - step)
        acted = [acts[block] for block in blocks]

        def columns(n, carry):
            at = pl.ds(pl.multiple_of(n * tile, tile), tile)
            for side in range(2):
                base = side * 2 * quarter + n * tile
                kept = jnp.dot(acted[side], down_w[:, pl.ds(pl.multiple_of(base + core * quarter, 128), tile)], preferred_element_type=jnp.float32)
                sent = jnp.dot(acted[side], down_w[:, pl.ds(pl.multiple_of(base + other * quarter, 128), tile)], preferred_element_type=jnp.float32)
                contrib[side, :, :, at] = kept.reshape(2, own_rows, tile)
                peer_out[side, step, :, :, at] = sent.reshape(2, own_rows, tile)
            return carry

        lax.fori_loop(0, quarter // tile, columns, 0)
        for side in range(2):
            swap_copy(side, step).start()

    def reduce_step(step):
        partial_sums(step)
        for side in range(2):
            swap_copy(side, step).wait_recv()
        for sub in range(2):
            for side in range(2):
                added = contrib[side, sub] + peer_in[side, step, sub]

                @pl.when(step == 0)
                def _(side=side, sub=sub, added=added):
                    ring[side, step, sub] = added

                @pl.when(step > 0)
                def _(side=side, sub=sub, added=added):
                    ring_copy(side, step - 1, sub).wait_recv()
                    ring[side, step, sub] = ring[side, step, sub] + added

                @pl.when(step < final)
                def _(side=side, sub=sub):
                    ring_copy(side, step, sub).start()

    def gather_step(hop, carry):
        last = hop == half_way
        for sub in range(2):
            for side in range(2):
                def arrive(side=side, sub=sub):
                    remote(rows_in.at[block_at(side, hop), core, sub], rows_in.at[block_at(side, hop), core, sub], ag_send.at[side, hop - 1, sub], ag_recv.at[side, hop - 1, sub], sides[side]).wait_recv()

                def forward(side=side, sub=sub):
                    hop_copy(side, hop + 1, sub).start()

                if side == sub:
                    arrive()
                    pl.when(jnp.logical_not(last))(forward)
                else:
                    pl.when(jnp.logical_not(last))(arrive)
                    pl.when(hop < half_way - 1)(forward)
        first = hop
        second = jnp.where(last, 0, chips - hop)
        peer_copy(first).start()

        @pl.when(jnp.logical_not(last))
        def _():
            peer_copy(second).start()

        peer_copy(first).wait_recv()
        peer_copy(second).wait_recv()
        for_first = rows_in[first].reshape(block_rows, width)
        for_second = rows_in[second].reshape(block_rows, width)
        both = jnp.concatenate([for_first, for_second], axis=0)

        def columns(n, carry):
            at = pl.ds(pl.multiple_of(n * tile, tile), tile)
            gate = jnp.dot(both, gate_w[:, at], preferred_element_type=jnp.float32)
            up = jnp.dot(both, up_w[:, at], preferred_element_type=jnp.float32)
            act = (jax.nn.silu(gate) * up).astype(jnp.bfloat16)
            acts[first, :, at] = act[:block_rows]
            acts[second, :, at] = act[block_rows:]
            return carry

        lax.fori_loop(0, hidden // tile, columns, 0)
        reduce_step(hop - 1)
        return carry

    lax.fori_loop(1, half_way + 1, gather_step, 0)

    def later_step(step, carry):
        reduce_step(step)
        return carry

    lax.fori_loop(half_way, chips, later_step, 0)

    def fin_copy(side):
        return remote(ring.at[side, final, other], fin_in.at[side], fin_send.at[side], fin_recv.at[side], peer)

    for side in range(2):
        fin_copy(side).start()
    for side in range(2):
        mine = pl.ds(pl.multiple_of((2 * side + core) * quarter, 128), quarter)
        o_ref[:, mine] = (r_ref[:, mine].astype(jnp.float32) + ring[side, final, core]).astype(jnp.bfloat16)
    for side in range(2):
        theirs = pl.ds(pl.multiple_of((2 * side + other) * quarter, 128), quarter)
        fin_copy(side).wait_recv()
        o_ref[:, theirs] = (r_ref[:, theirs].astype(jnp.float32) + fin_in[side]).astype(jnp.bfloat16)

    for side in range(2):
        fin_copy(side).wait_send()
        for sub in range(2):
            for hop in range(1, half_way + 1):
                if hop < half_way or side == sub:
                    hop_copy(side, hop, sub).wait_send()

    def drain(step, carry):
        for side in range(2):
            swap_copy(side, step).wait_send()
            for sub in range(2):
                pl.when(step < final)(lambda side=side, sub=sub: ring_copy(side, step, sub).wait_send())
        peer_copy(step).wait_send()
        return carry

    lax.fori_loop(0, chips, drain, 0)


def mlp_group(axis, devices, mlp_in, residual, w_gate, w_up, w_down):
    chips = devices // 2
    rows, width = mlp_in.shape
    hidden = w_gate.shape[1]
    quarter = width // 4
    dma = pltpu.SemaphoreType.DMA
    any_spec = pl.BlockSpec(memory_space=pl.ANY)
    vmem_spec = pl.BlockSpec(memory_space=pltpu.VMEM)
    return pl.pallas_call(
        functools.partial(mlp_kernel, axis, chips),
        in_specs=[vmem_spec, vmem_spec, any_spec, any_spec, any_spec],
        out_specs=vmem_spec,
        out_shape=jax.ShapeDtypeStruct((rows, width), jnp.bfloat16),
        scratch_shapes=[pltpu.VMEM((width, hidden), jnp.bfloat16), pltpu.VMEM((width, hidden), jnp.bfloat16), pltpu.VMEM((hidden, width), jnp.bfloat16),
                        pltpu.VMEM((chips, 2, 2, rows // 2, width), jnp.bfloat16), pltpu.VMEM((chips, 2 * rows, hidden), jnp.bfloat16),
                        pltpu.VMEM((2, chips, 2, rows, quarter), jnp.float32), pltpu.VMEM((2, chips, 2, rows, quarter), jnp.float32),
                        pltpu.VMEM((2, chips, 2, rows, quarter), jnp.float32), pltpu.VMEM((2, 2, rows, quarter), jnp.float32), pltpu.VMEM((2, rows, quarter), jnp.float32),
                        dma((3,)), dma((2, chips // 2, 2)), dma((2, chips // 2, 2)), dma((chips,)), dma((chips,)),
                        dma((2, chips, 2)), dma((2, chips, 2)), dma((2, chips)), dma((2, chips)), dma((2,)), dma((2,))],
        compiler_params=pltpu.CompilerParams(collective_id=0, has_side_effects=True, vmem_limit_bytes=VMEM_BYTES),
        name='mlp_group',
    )(mlp_in.reshape(2, rows // 2, width), residual, w_gate, w_up, w_down)


def pair_kernel(axis, eps, o_ref, x_ref, g_ref, w_hbm, r_ref, u_ref, o_all, x_in, r_out, r_in, acc, stream, load_sem, send_sem, recv_sem):
    me = lax.axis_index(axis)
    core = lax.rem(me, 2)
    other = 1 - core
    peer = me + 1 - 2 * core
    rows, width = x_ref.shape
    half = width // 2
    slots, depth = stream.shape[0], stream.shape[1]
    count = o_ref.shape[1] // depth
    mine = pl.ds(pl.multiple_of(core * half, 128), half)
    theirs = pl.ds(pl.multiple_of(other * half, 128), half)

    def load(step):
        slot = lax.rem(step, slots)
        return pltpu.make_async_copy(w_hbm.at[pl.ds(pl.multiple_of(step * depth, depth), depth), mine], stream.at[slot], load_sem.at[slot])

    for step in range(slots):
        load(step).start()
    barrier = pltpu.get_barrier_semaphore()
    pl.semaphore_signal(barrier, inc=1, device_id={axis: peer}, device_id_type=pl.DeviceIdType.MESH)
    pl.semaphore_wait(barrier, 1)

    def remote(src, dst, n):
        return pltpu.make_async_remote_copy(src_ref=src, dst_ref=dst, send_sem=send_sem.at[n], recv_sem=recv_sem.at[n], device_id={axis: peer}, device_id_type=pl.DeviceIdType.MESH)

    o_copy = remote(o_ref, o_all.at[core], 0)
    x_copy = remote(x_ref.at[:, theirs], x_in, 1)
    o_copy.start()
    x_copy.start()
    o_all[core] = o_ref[...]
    acc[...] = jnp.zeros_like(acc)
    o_copy.wait_recv()

    def body(step, carry):
        load(step).wait()
        heads = o_all[:, :, pl.ds(pl.multiple_of(step * depth, depth), depth)].reshape(2 * rows, depth)
        acc[...] += jnp.dot(heads, stream[lax.rem(step, slots)], preferred_element_type=jnp.float32).reshape(2, rows, half)

        @pl.when(step + slots < count)
        def _():
            load(step + slots).start()

        return carry

    lax.fori_loop(0, count, body, 0)
    x_copy.wait_recv()
    r_out[...] = (x_in[...].astype(jnp.float32) + acc[other]).astype(jnp.bfloat16)
    r_copy = remote(r_out, r_in, 2)
    r_copy.start()
    r_ref[:, mine] = (x_ref[:, mine].astype(jnp.float32) + acc[core]).astype(jnp.bfloat16)
    r_copy.wait_recv()
    r_ref[:, theirs] = r_in[...]
    whole = r_ref[...].astype(jnp.float32)
    mean_sq = jnp.mean(whole * whole, axis=-1, keepdims=True)
    u_ref[...] = (whole * lax.rsqrt(mean_sq + eps) * g_ref[...]).astype(jnp.bfloat16)
    o_copy.wait_send()
    x_copy.wait_send()
    r_copy.wait_send()


OUT_DEPTH = 1024
OUT_SLOTS = 4


def pair_out(axis, head_out, hidden, w_flat, norm_mlp):
    rows, depth = head_out.shape
    width = hidden.shape[1]
    half = width // 2
    dma = pltpu.SemaphoreType.DMA
    vmem_spec = pl.BlockSpec(memory_space=pltpu.VMEM)
    return pl.pallas_call(
        functools.partial(pair_kernel, axis, EPSILON),
        in_specs=[vmem_spec, vmem_spec, vmem_spec, pl.BlockSpec(memory_space=pl.ANY)],
        out_specs=[vmem_spec, vmem_spec],
        out_shape=[jax.ShapeDtypeStruct((rows, width), jnp.bfloat16)] * 2,
        scratch_shapes=[pltpu.VMEM((2, rows, depth), jnp.bfloat16), pltpu.VMEM((rows, half), jnp.bfloat16), pltpu.VMEM((rows, half), jnp.bfloat16),
                        pltpu.VMEM((rows, half), jnp.bfloat16), pltpu.VMEM((2, rows, half), jnp.float32), pltpu.VMEM((OUT_SLOTS, OUT_DEPTH, half), jnp.bfloat16),
                        dma((OUT_SLOTS,)), dma((3,)), dma((3,))],
        compiler_params=pltpu.CompilerParams(collective_id=1, has_side_effects=True, vmem_limit_bytes=VMEM_BYTES),
        name='pair_out',
    )(head_out, hidden, norm_mlp[None, :], w_flat)


def attention_rows(axis, hidden, ckv_cache, kpe_cache, cache_len, rope_cos, rope_sin, norm_attn, w_dq, norm_q, w_uq, w_dkv, norm_kv, w_uk, w_uv, w_out, norm_mlp):
    value_a7 = w_uk.shape[0]
    score_scale = MSCALE * MSCALE / math.sqrt(w_uq.shape[2])
    normed = rms_norm(hidden, norm_attn).astype(jnp.bfloat16)
    q_latent = rms_norm(jnp.dot(normed, w_dq, preferred_element_type=jnp.float32), norm_q).astype(jnp.bfloat16)
    q_nope, q_pe = q_project(q_latent, w_uq, rope_cos, rope_sin)
    kv_full = jnp.dot(normed, w_dkv, preferred_element_type=jnp.float32)
    ckv_new = rms_norm(kv_full[:, :value_a7], norm_kv).astype(jnp.bfloat16)
    kpe_new = apply_rope(kv_full[:, value_a7:], rope_cos, rope_sin).astype(jnp.bfloat16)
    q_abs = absorb(q_nope, w_uk)
    scores = (jnp.einsum('bhl,btl->bht', q_abs, ckv_cache, preferred_element_type=jnp.float32)
              + jnp.einsum('bhr,btr->bht', q_pe, kpe_cache, preferred_element_type=jnp.float32)) * score_scale
    positions = jnp.arange(ckv_cache.shape[1])
    scores = jnp.where(positions[None, None, :] < cache_len[:, None, None], scores, -jnp.inf)
    score_new = (jnp.einsum('bhl,bl->bh', q_abs, ckv_new, preferred_element_type=jnp.float32)
                 + jnp.einsum('bhr,br->bh', q_pe, kpe_new, preferred_element_type=jnp.float32)) * score_scale
    row_max = jnp.maximum(jnp.max(scores, axis=-1), score_new)
    exp_cache = jnp.exp(scores - row_max[..., None])
    exp_new = jnp.exp(score_new - row_max)
    norm_sum = jnp.sum(exp_cache, axis=-1) + exp_new
    weighted = (jnp.einsum('bht,btl->bhl', exp_cache.astype(jnp.bfloat16), ckv_cache, preferred_element_type=jnp.float32)
                + exp_new.astype(jnp.bfloat16).astype(jnp.float32)[..., None] * ckv_new.astype(jnp.float32)[:, None, :])
    lat_out = (weighted / norm_sum[..., None]).astype(jnp.bfloat16)
    head_out = value_heads(lat_out, w_uv)
    w_flat = w_out.reshape(w_out.shape[0] * w_out.shape[1], w_out.shape[2])
    residual, mlp_in = pair_out(axis, head_out, hidden, w_flat, norm_mlp)
    return residual, mlp_in, ckv_new, kpe_new


def solution(mesh):
    row_spec = P(('rep', 'dp'), None)
    cube_spec = P(('rep', 'dp'), None, None)
    full_spec = P()
    in_specs = (row_spec, cube_spec, cube_spec, P(('rep', 'dp')), row_spec, row_spec,
                full_spec, full_spec, full_spec, full_spec, full_spec, full_spec, full_spec, full_spec, full_spec, full_spec,
                P(None, 'dp'), P(None, 'dp'), P('dp', None))

    def local_step(hidden, ckv_cache, kpe_cache, cache_len, rope_cos, rope_sin, norm_attn, w_dq, norm_q, w_uq, w_dkv, norm_kv, w_uk, w_uv, w_out, norm_mlp, w_gate, w_up, w_down):
        residual, mlp_in, ckv_new, kpe_new = attention_rows('dp', hidden, ckv_cache, kpe_cache, cache_len, rope_cos, rope_sin, norm_attn, w_dq, norm_q, w_uq, w_dkv, norm_kv, w_uk, w_uv, w_out, norm_mlp)
        out_hidden = mlp_group('dp', mesh.shape['dp'], mlp_in, residual, w_gate, w_up, w_down)
        return out_hidden, ckv_new, kpe_new

    return jax.shard_map(local_step, mesh=mesh, in_specs=in_specs, out_specs=(row_spec, row_spec, row_spec), check_vma=False)
```

```python
import functools
import math
import jax
import jax.numpy as jnp
from jax import lax
from jax.experimental import pallas as pl
from jax.experimental.pallas import tpu as pltpu
from jax.sharding import PartitionSpec as P

EPSILON = 1e-6
MSCALE = 0.1 * math.log(40.0) + 1.0


def rms_norm(values_in, gain_vec):
    floats = values_in.astype(jnp.float32)
    mean_sq = jnp.mean(floats * floats, axis=-1, keepdims=True)
    return floats * lax.rsqrt(mean_sq + EPSILON) * gain_vec


def apply_rope(values_in, cos_t, sin_t):
    half_dim = values_in.shape[-1] // 2
    low_half = values_in[..., :half_dim]
    high_half = values_in[..., half_dim:]
    return jnp.concatenate([low_half * cos_t - high_half * sin_t, high_half * cos_t + low_half * sin_t], axis=-1)


GROUP = 8
Q_DEPTH = 4096
Q_PACK = 2
HEAD_PACK = 4
LANES = 128
VMEM_BYTES = 60 * 1024 * 1024


def lane_ids(shape, axis):
    return lax.broadcasted_iota(jnp.int32, shape, axis)


def q_kernel(cq_ref, cos_ref, sin_ref, wa_ref, wb_ref, oa_ref, ob_ref, spread):
    step = pl.program_id(0)
    rows, depth = cq_ref.shape
    wide = LANES * GROUP

    @pl.when(step == 0)
    def _():
        expand = (lane_ids((LANES, wide), 1) // GROUP == lane_ids((LANES, wide), 0)).astype(jnp.bfloat16)
        mine = lane_ids((rows, wide), 1) % GROUP == lane_ids((rows, wide), 0) % GROUP
        for k in range(depth // LANES):
            part = jnp.dot(cq_ref[:, k * LANES:(k + 1) * LANES], expand, preferred_element_type=jnp.float32)
            spread[:, k * wide:(k + 1) * wide] = jnp.where(mine, part, 0.0).astype(jnp.bfloat16)

    plain = step < pl.num_programs(0) * 2 // 3
    for part in range(Q_PACK):
        acc = jnp.zeros((rows, 2 * LANES), jnp.float32)
        count = Q_DEPTH // GROUP
        for at in range(0, depth, count):
            both = jnp.concatenate([wa_ref[at:at + count, part * GROUP:(part + 1) * GROUP, :].reshape(Q_DEPTH, LANES),
                                    wb_ref[at:at + count, part * GROUP:(part + 1) * GROUP, :].reshape(Q_DEPTH, LANES)], axis=1)
            acc = acc + jnp.dot(spread[:, at * GROUP:at * GROUP + Q_DEPTH], both, preferred_element_type=jnp.float32)
        low = acc[:, :LANES]
        high = acc[:, LANES:]
        cos_c = cos_ref[part]
        sin_c = sin_ref[part]
        first = jnp.where(plain, low, low * cos_c - high * sin_c)
        second = jnp.where(plain, high, high * cos_c + low * sin_c)
        batch = rows // GROUP
        oa_ref[:, part * GROUP:(part + 1) * GROUP, :] = first.reshape(batch, GROUP, LANES).astype(jnp.bfloat16)
        ob_ref[:, part * GROUP:(part + 1) * GROUP, :] = second.reshape(batch, GROUP, LANES).astype(jnp.bfloat16)


def q_project(repeated, w_uq, rope_cos, rope_sin):
    batch, depth = rope_cos.shape[0], repeated.shape[1]
    heads, width = w_uq.shape[1], w_uq.shape[2]
    stored = jnp.transpose(w_uq, (0, 2, 1))
    rows = batch * GROUP
    half = rope_cos.shape[1]
    turns = half // (GROUP * Q_PACK)
    nope = (width - 2 * half) // (2 * GROUP * Q_PACK)
    cos_c = rope_cos.reshape(batch, half // GROUP, GROUP).transpose(1, 0, 2).reshape(half // GROUP, rows, 1)
    sin_c = rope_sin.reshape(batch, half // GROUP, GROUP).transpose(1, 0, 2).reshape(half // GROUP, rows, 1)
    steps = nope + turns

    def first_at(j):
        return (0, jnp.where(j < nope, j, j + nope), 0)

    def second_at(j):
        return (0, jnp.where(j < nope, j + nope, j + nope + turns), 0)

    def turn_at(j):
        return (jnp.maximum(j - nope, 0), 0, 0)

    out_a, out_b = pl.pallas_call(
        q_kernel,
        grid=(steps,),
        in_specs=[pl.BlockSpec((rows, depth), lambda j: (0, 0)),
                  pl.BlockSpec((Q_PACK, rows, 1), turn_at), pl.BlockSpec((Q_PACK, rows, 1), turn_at),
                  pl.BlockSpec((depth, Q_PACK * GROUP, heads), first_at), pl.BlockSpec((depth, Q_PACK * GROUP, heads), second_at)],
        out_specs=[pl.BlockSpec((batch, Q_PACK * GROUP, heads), lambda j: (0, j, 0))] * 2,
        out_shape=[jax.ShapeDtypeStruct((batch, steps * Q_PACK * GROUP, heads), jnp.bfloat16)] * 2,
        scratch_shapes=[pltpu.VMEM((rows, depth * GROUP), jnp.bfloat16)],
        compiler_params=pltpu.CompilerParams(vmem_limit_bytes=VMEM_BYTES),
        cost_estimate=pl.CostEstimate(flops=2 * batch * depth * heads * width, bytes_accessed=2 * depth * heads * width, transcendentals=0),
        name='q_project',
    )(repeated, cos_c, sin_c, stored, stored)
    return out_a, out_b


def absorb_kernel(a_ref, b_ref, w_ref, o_ref, plain, turned):
    batch, half, heads = a_ref.shape
    packed = turned.shape[2]
    outer, inner = w_ref.shape[0], w_ref.shape[2]
    rows = batch * GROUP
    own = lane_ids((rows, inner), 0) % GROUP
    step = pl.program_id(0)

    @pl.when(step == 0)
    def _():
        def turn(row, carry):
            flat = jnp.concatenate([a_ref[row], b_ref[row]], axis=0).astype(jnp.float32).T.astype(jnp.bfloat16)
            for part in range(heads // packed):
                turned[part, row] = flat[part * packed:(part + 1) * packed, :]
            return carry

        lax.fori_loop(0, batch, turn, 0)

    for part in range(packed // GROUP):
        span = slice(part * GROUP, (part + 1) * GROUP)
        plain[part] = w_ref[:, span, :].reshape(outer * GROUP, inner).astype(jnp.float32)
        queries = turned[step, :, span, :].reshape(rows, inner)
        acc = jnp.zeros((rows, outer), jnp.float32)
        for h in range(0, GROUP, 2):
            left = jnp.concatenate([jnp.where(own == h, queries, jnp.zeros_like(queries)),
                                    jnp.where(own == h + 1, queries, jnp.zeros_like(queries))], axis=1)
            right = jnp.concatenate([plain[part, pl.ds(h, outer, stride=GROUP), :].astype(jnp.bfloat16),
                                     plain[part, pl.ds(h + 1, outer, stride=GROUP), :].astype(jnp.bfloat16)], axis=1)
            acc = acc + lax.dot_general(left, right, (((1,), (1,)), ((), ())), preferred_element_type=jnp.float32)
        o_ref[:, span, :] = acc.reshape(batch, GROUP, outer).astype(jnp.bfloat16)


def absorb(out_a, out_b, w_uk):
    batch, heads = out_a.shape[0], out_a.shape[2]
    outer, inner = w_uk.shape[0], w_uk.shape[2]
    packed = HEAD_PACK * GROUP
    half_spec = pl.BlockSpec((batch, inner // 2, heads), lambda g: (0, 0, 0))
    return pl.pallas_call(
        absorb_kernel,
        grid=(heads // packed,),
        in_specs=[half_spec, half_spec, pl.BlockSpec((outer, packed, inner), lambda g: (0, g, 0))],
        out_specs=pl.BlockSpec((batch, packed, outer), lambda g: (0, g, 0)),
        out_shape=jax.ShapeDtypeStruct((batch, heads, outer), jnp.bfloat16),
        scratch_shapes=[pltpu.VMEM((HEAD_PACK, outer * GROUP, inner), jnp.float32), pltpu.VMEM((heads // packed, batch, packed, inner), jnp.bfloat16)],
        compiler_params=pltpu.CompilerParams(vmem_limit_bytes=VMEM_BYTES),
        cost_estimate=pl.CostEstimate(flops=2 * batch * heads * inner * outer, bytes_accessed=2 * heads * inner * outer, transcendentals=0),
        name='absorb',
    )(out_a, out_b, w_uk)


REQUESTS = 8
TOGETHER = 4


def attend_kernel(scale, len_ref, q_ref, ra_ref, rb_ref, ckv_ref, kpe_ref, c_ref, k_ref, o_ref):
    count = q_ref.shape[0]
    base = pl.program_id(0) * count
    for start in range(0, count, TOGETHER):
        group = range(start, start + TOGETHER)
        rotary = {i: jnp.concatenate([ra_ref[i], rb_ref[i]], axis=0).astype(jnp.float32).T for i in group}
        scores = {i: (lax.dot_general(q_ref[i], ckv_ref[i], (((1,), (1,)), ((), ())), preferred_element_type=jnp.float32)
                      + jnp.dot(rotary[i].astype(jnp.bfloat16), kpe_ref[i], preferred_element_type=jnp.float32)) * scale for i in group}
        fresh = {i: c_ref[i:i + 1, :] for i in group}
        score_new = {i: (jnp.sum(q_ref[i].astype(jnp.float32) * fresh[i], axis=-1, keepdims=True)
                         + jnp.sum(rotary[i] * k_ref[i:i + 1, :], axis=-1, keepdims=True)) * scale for i in group}
        scores = {i: jnp.where(lane_ids(scores[i].shape, 1) < len_ref[base + i], scores[i], -jnp.inf) for i in group}
        row_max = {i: jnp.maximum(jnp.max(scores[i], axis=-1, keepdims=True), score_new[i]) for i in group}
        exp_cache = {i: jnp.exp(scores[i] - row_max[i]) for i in group}
        exp_new = {i: jnp.exp(score_new[i] - row_max[i]) for i in group}
        weighted = {i: jnp.dot(exp_cache[i].astype(jnp.bfloat16), ckv_ref[i], preferred_element_type=jnp.float32) for i in group}
        norm_sum = {i: jnp.sum(exp_cache[i], axis=-1, keepdims=True) + exp_new[i] for i in group}
        for i in group:
            total = weighted[i] + exp_new[i].astype(jnp.bfloat16).astype(jnp.float32) * fresh[i]
            o_ref[i] = (total / norm_sum[i]).astype(jnp.bfloat16)


def attend(scale, q_abs, out_a, out_b, ckv_cache, kpe_cache, cache_len, ckv_new, kpe_new):
    batch, heads, outer = q_abs.shape
    past, rotary = kpe_cache.shape[1], kpe_cache.shape[2]
    half = rotary // 2
    last = out_a.shape[1] // half - 1
    turn_spec = pl.BlockSpec((REQUESTS, half, heads), lambda b: (b, last, 0))
    return pl.pallas_call(
        functools.partial(attend_kernel, scale),
        grid=(batch // REQUESTS,),
        in_specs=[pl.BlockSpec(memory_space=pltpu.SMEM), pl.BlockSpec((REQUESTS, heads, outer), lambda b: (b, 0, 0)), turn_spec, turn_spec,
                  pl.BlockSpec((REQUESTS, past, outer), lambda b: (b, 0, 0)), pl.BlockSpec((REQUESTS, rotary, past), lambda b: (b, 0, 0)),
                  pl.BlockSpec((REQUESTS, outer), lambda b: (b, 0)), pl.BlockSpec((REQUESTS, rotary), lambda b: (b, 0))],
        out_specs=pl.BlockSpec((REQUESTS, heads, outer), lambda b: (b, 0, 0)),
        out_shape=jax.ShapeDtypeStruct((batch, heads, outer), jnp.bfloat16),
        compiler_params=pltpu.CompilerParams(vmem_limit_bytes=VMEM_BYTES),
        cost_estimate=pl.CostEstimate(flops=4 * batch * heads * past * outer, bytes_accessed=2 * batch * past * outer, transcendentals=0),
        name='attend',
    )(cache_len, q_abs, out_a, out_b, ckv_cache, kpe_cache.transpose(0, 2, 1), ckv_new, kpe_new)


FRONT_DEPTH = 1024


def front_kernel(x_ref, g_ref, wq_ref, wkv_ref, gq_ref, gkv_ref, cos_ref, sin_ref, q_ref, c_ref, k_ref, c_wide, k_wide, normed, q_acc, kv_acc):
    step = pl.program_id(0)
    depth = wq_ref.shape[0]

    @pl.when(step == 0)
    def _():
        normed[...] = rms_norm(x_ref[...], g_ref[...]).astype(jnp.bfloat16)
        q_acc[...] = jnp.zeros_like(q_acc)
        kv_acc[...] = jnp.zeros_like(kv_acc)

    part = normed[:, pl.ds(pl.multiple_of(step * depth, depth), depth)]
    q_acc[...] += jnp.dot(part, wq_ref[...], preferred_element_type=jnp.float32)
    kv_acc[...] += lax.dot_general(part, wkv_ref[...], (((1,), (1,)), ((), ())), preferred_element_type=jnp.float32)

    @pl.when(step == pl.num_programs(0) - 1)
    def _():
        q_latent = rms_norm(q_acc[...], gq_ref[...]).astype(jnp.bfloat16)
        rows = (q_ref.shape[0], q_latent.shape[0])
        repeat = (lane_ids(rows, 0) // GROUP == lane_ids(rows, 1)).astype(jnp.bfloat16)
        q_ref[...] = jnp.dot(repeat, q_latent, preferred_element_type=jnp.float32).astype(jnp.bfloat16)
        inner = c_ref.shape[1]
        kv = kv_acc[...]
        c_new = rms_norm(kv[:, :inner], gkv_ref[...]).astype(jnp.bfloat16)
        k_new = apply_rope(kv[:, inner:], cos_ref[...], sin_ref[...]).astype(jnp.bfloat16)
        c_ref[...] = c_new
        k_ref[...] = k_new
        c_wide[...] = c_new.astype(jnp.float32)
        k_wide[...] = k_new.astype(jnp.float32)


def front(hidden, rope_cos, rope_sin, norm_attn, w_dq, norm_q, w_dkv, norm_kv):
    batch, width = hidden.shape
    latent = w_dq.shape[1]
    joint = w_dkv.shape[1]
    inner = norm_kv.shape[0]

    def whole(*shape):
        return pl.BlockSpec(shape, lambda k: (0,) * len(shape))

    half = rope_cos.shape[1]
    return pl.pallas_call(
        front_kernel,
        grid=(width // FRONT_DEPTH,),
        in_specs=[whole(batch, width), whole(1, width), pl.BlockSpec((FRONT_DEPTH, latent), lambda k: (k, 0)), pl.BlockSpec((joint, FRONT_DEPTH), lambda k: (0, k)),
                  whole(1, latent), whole(1, inner), whole(batch, half), whole(batch, half)],
        out_specs=[whole(batch * GROUP, latent)] + [whole(batch, inner), whole(batch, joint - inner)] * 2,
        out_shape=[jax.ShapeDtypeStruct((batch * GROUP, latent), jnp.bfloat16)] + [jax.ShapeDtypeStruct((batch, size), kind) for kind in (jnp.bfloat16, jnp.float32) for size in (inner, joint - inner)],
        scratch_shapes=[pltpu.VMEM((batch, width), jnp.bfloat16), pltpu.VMEM((batch, latent), jnp.float32), pltpu.VMEM((batch, joint), jnp.float32)],
        compiler_params=pltpu.CompilerParams(vmem_limit_bytes=VMEM_BYTES),
        name='front',
    )(hidden, norm_attn[None, :], w_dq, w_dkv.T, norm_q[None, :], norm_kv[None, :], rope_cos, rope_sin)


def value_kernel(l_ref, w_ref, o_ref, plain, picked):
    batch, heads, outer = l_ref.shape
    inner = w_ref.shape[2]
    rows = batch * GROUP
    own = lane_ids((rows, inner), 0) % GROUP
    for part in range(heads // GROUP):
        span = slice(part * GROUP, (part + 1) * GROUP)
        plain[part] = w_ref[:, span, :].reshape(outer * GROUP, inner).astype(jnp.float32)
        latents = l_ref[:, span, :].reshape(rows, outer)
        acc = jnp.zeros((rows, inner), jnp.float32)
        for h in range(0, GROUP, 2):
            right = jnp.concatenate([plain[part, pl.ds(h, outer, stride=GROUP), :].astype(jnp.bfloat16),
                                     plain[part, pl.ds(h + 1, outer, stride=GROUP), :].astype(jnp.bfloat16)], axis=1)
            both = jnp.dot(latents, right, preferred_element_type=jnp.float32)
            acc = jnp.where(own == h, both[:, :inner], jnp.where(own == h + 1, both[:, inner:], acc))
        picked[part] = acc
        for h in range(GROUP):
            o_ref[:, (part * GROUP + h) * inner:(part * GROUP + h + 1) * inner] = picked[part, pl.ds(h, batch, stride=GROUP), :].astype(jnp.bfloat16)


def value_heads(lat_out, w_uv):
    batch, heads, outer = lat_out.shape
    inner = w_uv.shape[2]
    return pl.pallas_call(
        value_kernel,
        grid=(heads // (HEAD_PACK * GROUP),),
        in_specs=[pl.BlockSpec((batch, HEAD_PACK * GROUP, outer), lambda g: (0, g, 0)),
                  pl.BlockSpec((outer, HEAD_PACK * GROUP, inner), lambda g: (0, g, 0))],
        out_specs=pl.BlockSpec((batch, HEAD_PACK * GROUP * inner), lambda g: (0, g)),
        out_shape=jax.ShapeDtypeStruct((batch, heads * inner), jnp.bfloat16),
        scratch_shapes=[pltpu.VMEM((HEAD_PACK, outer * GROUP, inner), jnp.float32), pltpu.VMEM((HEAD_PACK, batch * GROUP, inner), jnp.float32)],
        compiler_params=pltpu.CompilerParams(vmem_limit_bytes=VMEM_BYTES),
        cost_estimate=pl.CostEstimate(flops=2 * batch * heads * inner * outer, bytes_accessed=2 * heads * inner * outer, transcendentals=0),
        name='value_heads',
    )(lat_out, w_uv)


def mlp_kernel(axis, chips, u_ref, r_ref, gate_hbm, up_hbm, down_hbm, o_ref, gate_w, up_w, down_w, rows_in, acts, ring, peer_out, peer_in, contrib, fin_in,
               load_sem, ag_send, ag_recv, pe_send, pe_recv, rs_send, rs_recv, px_send, px_recv, fin_send, fin_recv):
    me = lax.axis_index(axis)
    core = lax.rem(me, 2)
    other = 1 - core
    chip = lax.div(me, 2)
    peer = chip * 2 + other
    ahead = lax.rem(chip + 1, chips) * 2 + core
    behind = lax.rem(chip + chips - 1, chips) * 2 + core
    sides = (ahead, behind)
    half_way = chips // 2
    width = u_ref.shape[-1]
    quarter = width // 4
    tile = 256
    sub_rows = u_ref.shape[1]
    own_rows = 2 * sub_rows
    block_rows = 2 * own_rows
    hidden = gate_w.shape[1]

    loads = [pltpu.make_async_copy(src, dst, load_sem.at[n]) for n, (src, dst) in enumerate(((gate_hbm, gate_w), (up_hbm, up_w), (down_hbm, down_w)))]
    for load in loads:
        load.start()

    barrier = pltpu.get_barrier_semaphore()
    for device in (ahead, behind, peer):
        pl.semaphore_signal(barrier, inc=1, device_id={axis: device}, device_id_type=pl.DeviceIdType.MESH)
    pl.semaphore_wait(barrier, 3)

    def remote(src, dst, send, recv, device):
        return pltpu.make_async_remote_copy(src_ref=src, dst_ref=dst, send_sem=send, recv_sem=recv, device_id={axis: device}, device_id_type=pl.DeviceIdType.MESH)

    def block_at(side, hop):
        return hop if side == 0 else lax.rem(chips - hop, chips)

    def hop_copy(side, hop, sub):
        src = u_ref.at[sub] if isinstance(hop, int) and hop == 1 else rows_in.at[block_at(side, hop - 1), core, sub]
        return remote(src, rows_in.at[block_at(side, hop), core, sub], ag_send.at[side, hop - 1, sub], ag_recv.at[side, hop - 1, sub], sides[side])

    def peer_copy(block):
        src = u_ref if isinstance(block, int) and block == 0 else rows_in.at[block, core]
        return remote(src, rows_in.at[block, core], pe_send.at[block], pe_recv.at[block], peer)

    for sub in range(2):
        for side in range(2):
            hop_copy(side, 1, sub).start()
    peer_copy(0).start()
    rows_in[0, core] = u_ref[...]
    for load in loads:
        load.wait()

    final = chips - 1

    def swap_copy(side, step):
        return remote(peer_out.at[side, step], peer_in.at[side, step], px_send.at[side, step], px_recv.at[side, step], peer)

    def ring_copy(side, step, sub):
        return remote(ring.at[side, step, sub], ring.at[side, step + 1, sub], rs_send.at[side, step, sub], rs_recv.at[side, step, sub], sides[side])

    def partial_sums(step):
        blocks = (lax.rem(step + 1, chips), chips - 1 - step)
        acted = [acts[block] for block in blocks]

        def columns(n, carry):
            at = pl.ds(pl.multiple_of(n * tile, tile), tile)
            for side in range(2):
                base = side * 2 * quarter + n * tile
                kept = jnp.dot(acted[side], down_w[:, pl.ds(pl.multiple_of(base + core * quarter, 128), tile)], preferred_element_type=jnp.float32)
                sent = jnp.dot(acted[side], down_w[:, pl.ds(pl.multiple_of(base + other * quarter, 128), tile)], preferred_element_type=jnp.float32)
                contrib[side, :, :, at] = kept.reshape(2, own_rows, tile)
                peer_out[side, step, :, :, at] = sent.reshape(2, own_rows, tile)
            return carry

        lax.fori_loop(0, quarter // tile, columns, 0)
        for side in range(2):
            swap_copy(side, step).start()

    def reduce_step(step):
        partial_sums(step)
        for side in range(2):
            swap_copy(side, step).wait_recv()
        for sub in range(2):
            for side in range(2):
                added = contrib[side, sub] + peer_in[side, step, sub]

                @pl.when(step == 0)
                def _(side=side, sub=sub, added=added):
                    ring[side, step, sub] = added

                @pl.when(step > 0)
                def _(side=side, sub=sub, added=added):
                    ring_copy(side, step - 1, sub).wait_recv()
                    ring[side, step, sub] = ring[side, step, sub] + added

                @pl.when(step < final)
                def _(side=side, sub=sub):
                    ring_copy(side, step, sub).start()

    def gather_step(hop, carry):
        last = hop == half_way
        for sub in range(2):
            for side in range(2):
                def arrive(side=side, sub=sub):
                    remote(rows_in.at[block_at(side, hop), core, sub], rows_in.at[block_at(side, hop), core, sub], ag_send.at[side, hop - 1, sub], ag_recv.at[side, hop - 1, sub], sides[side]).wait_recv()

                def forward(side=side, sub=sub):
                    hop_copy(side, hop + 1, sub).start()

                if side == sub:
                    arrive()
                    pl.when(jnp.logical_not(last))(forward)
                else:
                    pl.when(jnp.logical_not(last))(arrive)
                    pl.when(hop < half_way - 1)(forward)
        first = hop
        second = jnp.where(last, 0, chips - hop)
        peer_copy(first).start()

        @pl.when(jnp.logical_not(last))
        def _():
            peer_copy(second).start()

        peer_copy(first).wait_recv()
        peer_copy(second).wait_recv()
        for_first = rows_in[first].reshape(block_rows, width)
        for_second = rows_in[second].reshape(block_rows, width)
        both = jnp.concatenate([for_first, for_second], axis=0)

        def columns(n, carry):
            at = pl.ds(pl.multiple_of(n * tile, tile), tile)
            gate = jnp.dot(both, gate_w[:, at], preferred_element_type=jnp.float32)
            up = jnp.dot(both, up_w[:, at], preferred_element_type=jnp.float32)
            act = (jax.nn.silu(gate) * up).astype(jnp.bfloat16)
            acts[first, :, at] = act[:block_rows]
            acts[second, :, at] = act[block_rows:]
            return carry

        lax.fori_loop(0, hidden // tile, columns, 0)
        reduce_step(hop - 1)
        return carry

    lax.fori_loop(1, half_way + 1, gather_step, 0)

    def later_step(step, carry):
        reduce_step(step)
        return carry

    lax.fori_loop(half_way, chips, later_step, 0)

    def fin_copy(side):
        return remote(ring.at[side, final, other], fin_in.at[side], fin_send.at[side], fin_recv.at[side], peer)

    for side in range(2):
        fin_copy(side).start()
    for side in range(2):
        mine = pl.ds(pl.multiple_of((2 * side + core) * quarter, 128), quarter)
        o_ref[:, mine] = (r_ref[:, mine].astype(jnp.float32) + ring[side, final, core]).astype(jnp.bfloat16)
    for side in range(2):
        theirs = pl.ds(pl.multiple_of((2 * side + other) * quarter, 128), quarter)
        fin_copy(side).wait_recv()
        o_ref[:, theirs] = (r_ref[:, theirs].astype(jnp.float32) + fin_in[side]).astype(jnp.bfloat16)

    for side in range(2):
        fin_copy(side).wait_send()
        for sub in range(2):
            for hop in range(1, half_way + 1):
                if hop < half_way or side == sub:
                    hop_copy(side, hop, sub).wait_send()

    def drain(step, carry):
        for side in range(2):
            swap_copy(side, step).wait_send()
            for sub in range(2):
                pl.when(step < final)(lambda side=side, sub=sub: ring_copy(side, step, sub).wait_send())
        peer_copy(step).wait_send()
        return carry

    lax.fori_loop(0, chips, drain, 0)


def mlp_group(axis, devices, mlp_in, residual, w_gate, w_up, w_down):
    chips = devices // 2
    rows, width = mlp_in.shape
    hidden = w_gate.shape[1]
    quarter = width // 4
    dma = pltpu.SemaphoreType.DMA
    any_spec = pl.BlockSpec(memory_space=pl.ANY)
    vmem_spec = pl.BlockSpec(memory_space=pltpu.VMEM)
    return pl.pallas_call(
        functools.partial(mlp_kernel, axis, chips),
        in_specs=[vmem_spec, vmem_spec, any_spec, any_spec, any_spec],
        out_specs=vmem_spec,
        out_shape=jax.ShapeDtypeStruct((rows, width), jnp.bfloat16),
        scratch_shapes=[pltpu.VMEM((width, hidden), jnp.bfloat16), pltpu.VMEM((width, hidden), jnp.bfloat16), pltpu.VMEM((hidden, width), jnp.bfloat16),
                        pltpu.VMEM((chips, 2, 2, rows // 2, width), jnp.bfloat16), pltpu.VMEM((chips, 2 * rows, hidden), jnp.bfloat16),
                        pltpu.VMEM((2, chips, 2, rows, quarter), jnp.float32), pltpu.VMEM((2, chips, 2, rows, quarter), jnp.float32),
                        pltpu.VMEM((2, chips, 2, rows, quarter), jnp.float32), pltpu.VMEM((2, 2, rows, quarter), jnp.float32), pltpu.VMEM((2, rows, quarter), jnp.float32),
                        dma((3,)), dma((2, chips // 2, 2)), dma((2, chips // 2, 2)), dma((chips,)), dma((chips,)),
                        dma((2, chips, 2)), dma((2, chips, 2)), dma((2, chips)), dma((2, chips)), dma((2,)), dma((2,))],
        compiler_params=pltpu.CompilerParams(collective_id=0, has_side_effects=True, vmem_limit_bytes=VMEM_BYTES),
        name='mlp_group',
    )(mlp_in.reshape(2, rows // 2, width), residual, w_gate, w_up, w_down)


def pair_kernel(axis, eps, o_ref, x_ref, g_ref, w_hbm, r_ref, u_ref, o_all, x_in, r_out, r_in, acc, stream, load_sem, send_sem, recv_sem):
    me = lax.axis_index(axis)
    core = lax.rem(me, 2)
    other = 1 - core
    peer = me + 1 - 2 * core
    rows, width = x_ref.shape
    half = width // 2
    slots, depth = stream.shape[0], stream.shape[1]
    count = o_ref.shape[1] // depth
    mine = pl.ds(pl.multiple_of(core * half, 128), half)
    theirs = pl.ds(pl.multiple_of(other * half, 128), half)

    def load(step):
        slot = lax.rem(step, slots)
        return pltpu.make_async_copy(w_hbm.at[pl.ds(pl.multiple_of(step * depth, depth), depth), mine], stream.at[slot], load_sem.at[slot])

    for step in range(slots):
        load(step).start()
    barrier = pltpu.get_barrier_semaphore()
    pl.semaphore_signal(barrier, inc=1, device_id={axis: peer}, device_id_type=pl.DeviceIdType.MESH)
    pl.semaphore_wait(barrier, 1)

    def remote(src, dst, n):
        return pltpu.make_async_remote_copy(src_ref=src, dst_ref=dst, send_sem=send_sem.at[n], recv_sem=recv_sem.at[n], device_id={axis: peer}, device_id_type=pl.DeviceIdType.MESH)

    o_copy = remote(o_ref, o_all.at[core], 0)
    x_copy = remote(x_ref.at[:, theirs], x_in, 1)
    o_copy.start()
    x_copy.start()
    o_all[core] = o_ref[...]
    acc[...] = jnp.zeros_like(acc)
    o_copy.wait_recv()

    def body(step, carry):
        load(step).wait()
        heads = o_all[:, :, pl.ds(pl.multiple_of(step * depth, depth), depth)].reshape(2 * rows, depth)
        acc[...] += jnp.dot(heads, stream[lax.rem(step, slots)], preferred_element_type=jnp.float32).reshape(2, rows, half)

        @pl.when(step + slots < count)
        def _():
            load(step + slots).start()

        return carry

    lax.fori_loop(0, count, body, 0)
    x_copy.wait_recv()
    r_out[...] = (x_in[...].astype(jnp.float32) + acc[other]).astype(jnp.bfloat16)
    r_copy = remote(r_out, r_in, 2)
    r_copy.start()
    r_ref[:, mine] = (x_ref[:, mine].astype(jnp.float32) + acc[core]).astype(jnp.bfloat16)
    r_copy.wait_recv()
    r_ref[:, theirs] = r_in[...]
    whole = r_ref[...].astype(jnp.float32)
    mean_sq = jnp.mean(whole * whole, axis=-1, keepdims=True)
    u_ref[...] = (whole * lax.rsqrt(mean_sq + eps) * g_ref[...]).astype(jnp.bfloat16)
    o_copy.wait_send()
    x_copy.wait_send()
    r_copy.wait_send()


OUT_DEPTH = 1024
OUT_SLOTS = 4


def pair_out(axis, head_out, hidden, w_flat, norm_mlp):
    rows, depth = head_out.shape
    width = hidden.shape[1]
    half = width // 2
    dma = pltpu.SemaphoreType.DMA
    vmem_spec = pl.BlockSpec(memory_space=pltpu.VMEM)
    return pl.pallas_call(
        functools.partial(pair_kernel, axis, EPSILON),
        in_specs=[vmem_spec, vmem_spec, vmem_spec, pl.BlockSpec(memory_space=pl.ANY)],
        out_specs=[vmem_spec, vmem_spec],
        out_shape=[jax.ShapeDtypeStruct((rows, width), jnp.bfloat16)] * 2,
        scratch_shapes=[pltpu.VMEM((2, rows, depth), jnp.bfloat16), pltpu.VMEM((rows, half), jnp.bfloat16), pltpu.VMEM((rows, half), jnp.bfloat16),
                        pltpu.VMEM((rows, half), jnp.bfloat16), pltpu.VMEM((2, rows, half), jnp.float32), pltpu.VMEM((OUT_SLOTS, OUT_DEPTH, half), jnp.bfloat16),
                        dma((OUT_SLOTS,)), dma((3,)), dma((3,))],
        compiler_params=pltpu.CompilerParams(collective_id=1, has_side_effects=True, vmem_limit_bytes=VMEM_BYTES),
        name='pair_out',
    )(head_out, hidden, norm_mlp[None, :], w_flat)


def attention_heads(hidden, ckv_cache, kpe_cache, cache_len, rope_cos, rope_sin, norm_attn, w_dq, norm_q, w_uq, w_dkv, norm_kv, w_uk, w_uv):
    score_scale = MSCALE * MSCALE / math.sqrt(w_uq.shape[2])
    repeated, ckv_new, kpe_new, ckv_wide, kpe_wide = front(hidden, rope_cos, rope_sin, norm_attn, w_dq, norm_q, w_dkv, norm_kv)
    out_a, out_b = q_project(repeated, w_uq, rope_cos, rope_sin)
    q_abs = absorb(out_a, out_b, w_uk)
    lat_out = attend(score_scale, q_abs, out_a, out_b, ckv_cache, kpe_cache, cache_len, ckv_wide, kpe_wide)
    return value_heads(lat_out, w_uv), ckv_new, kpe_new


def solution(mesh):
    row_spec = P(('rep', 'dp'), None)
    cube_spec = P(('rep', 'dp'), None, None)
    full_spec = P()
    in_specs = (row_spec, cube_spec, cube_spec, P(('rep', 'dp')), row_spec, row_spec,
                full_spec, full_spec, full_spec, full_spec, full_spec, full_spec, full_spec, full_spec, full_spec, full_spec,
                P(None, 'dp'), P(None, 'dp'), P('dp', None))

    def local_step(hidden, ckv_cache, kpe_cache, cache_len, rope_cos, rope_sin, norm_attn, w_dq, norm_q, w_uq, w_dkv, norm_kv, w_uk, w_uv, w_out, norm_mlp, w_gate, w_up, w_down):
        head_out, ckv_new, kpe_new = attention_heads(hidden, ckv_cache, kpe_cache, cache_len, rope_cos, rope_sin, norm_attn, w_dq, norm_q, w_uq, w_dkv, norm_kv, w_uk, w_uv)
        w_flat = w_out.reshape(w_out.shape[0] * w_out.shape[1], w_out.shape[2])
        residual, mlp_in = pair_out('dp', head_out, hidden, w_flat, norm_mlp)
        out_hidden = mlp_group('dp', mesh.shape['dp'], mlp_in, residual, w_gate, w_up, w_down)
        return out_hidden, ckv_new, kpe_new

    return jax.shard_map(local_step, mesh=mesh, in_specs=in_specs, out_specs=(row_spec, row_spec, row_spec), check_vma=False)
```
